128 devices in a mesh: pts: 128 (over z, y, x, core).
Axes of the slice: x: 4, y: 4, z: 4, core: 2. Of those that a mesh axis runs over, the one named last changes fastest.
Arguments:
- points: bfloat16 [65536, 64], P('pts'), may hold values from -10 to 10, as said below
- targets: float32 [65536], P('pts'), may hold values from -6 to 6
- ridge_weight: float32 [], replicated, may hold values from 0.5 to 4
Outputs:
- coefficients: float32 [65536], P('pts')
- residual: float32 [65536], P('pts')
The draws below stay inside these ranges and needn't reach their ends.
Inputs may be any that keep to these rules, and one draw needn't show every extreme that they name: `points`: each point lies near one of 1365 cluster centres; every coordinate is within -10 and 10.
All inputs are finite; a program needn't handle non-finite values.
Results may differ from the reference program's by a relative error of at most 0.005.
Values may be sent and summed in bfloat16 or wider, within the bound.
A program may use at most 192 MiB of HBM per device.

```python
import math
import jax
import jax.numpy as jnp
from jax import lax

D = 64
PTS_DEV = 512
ITERS = 2
NPTS = 65536
CLUSTERS = 1365


def draw_points(key, part):
    key_centre = jax.random.fold_in(key, 11)
    key_member = jax.random.fold_in(key, 12)
    key_noise = jax.random.fold_in(key, 13)
    centres = 0.5 * jax.random.truncated_normal(key_centre, -4.0, 4.0, (CLUSTERS, D), jnp.float32)
    members = jax.random.randint(key_member, (NPTS,), 0, CLUSTERS)
    noise = 0.5 * jax.random.truncated_normal(key_noise, -4.0, 4.0, (NPTS, D), jnp.float32)
    return (centres[members] + noise).astype(jnp.bfloat16)


def level_of(rng, dims, pieces, smallest, high):
    def one(axis_at, shards_of):
        steps = jax.random.uniform(jax.random.fold_in(jax.random.fold_in(rng, 6), axis_at), (shards_of,), jnp.float32, smallest / len(pieces), high / len(pieces))
        return jnp.repeat(jnp.exp(steps), dims[axis_at] // shards_of).reshape((-1,) + (1,) * (len(dims) - axis_at - 1))

    factor_of = one(*pieces[0])
    for cut in pieces[1:]:
        factor_of = factor_of * one(*cut)
    return factor_of


def normal_values(own_key, dims, scale, bound, split=(), kind=jnp.bfloat16):
    result = scale * jax.random.normal(own_key, dims, jnp.float32)
    if split:
        result = result * level_of(own_key, dims, split, -0.22, 0.18)
    return jnp.clip(result, -bound, bound).astype(kind)


def setup_inputs(seed: int = 0) -> dict:
    arg_keys = jax.random.split(jax.random.key(seed), 4)
    points = draw_points(jax.random.fold_in(arg_keys[3], 71), 0)
    targets = normal_values(arg_keys[1], (NPTS,), 1.0, 6.0, ((0, 128),), jnp.float32)
    ridge_weight = jnp.clip(jnp.exp(jax.random.uniform(arg_keys[2], (), jnp.float32, math.log(0.5), math.log(4.0))), 0.5, 4.0)
    return dict(points=points, targets=targets, ridge_weight=ridge_weight)


def reference(points, targets, ridge_weight):
    inverse_width = 1.0 / D
    widened = points.astype(jnp.float32)
    squared = jnp.sum(widened * widened, axis=1)
    blocks = points.reshape(NPTS // PTS_DEV, PTS_DEV, D)
    block_norms = squared.reshape(NPTS // PTS_DEV, PTS_DEV)

    def apply_operator(vector):
        vector_low = vector.astype(jnp.bfloat16)

        def tile_product(operands):
            tile_rows, tile_norms = operands
            cross_term = jnp.dot(tile_rows, points.T, preferred_element_type=jnp.float32)
            distance = tile_norms[:, None] + squared[None, :] - 2.0 * cross_term
            kernel = jnp.exp(-inverse_width * distance).astype(jnp.bfloat16)
            return jnp.dot(kernel, vector_low, preferred_element_type=jnp.float32)

        summed = lax.map(tile_product, (blocks, block_norms)).reshape(NPTS)
        return summed + ridge_weight * vector

    coefficients = jnp.zeros_like(targets)
    residual = targets
    direction = targets
    norm_now = jnp.sum(residual * residual)
    for iteration in range(ITERS):
        applied = apply_operator(direction)
        step_size = norm_now / jnp.sum(direction * applied)
        coefficients = coefficients + step_size * direction
        residual = residual - step_size * applied
        norm_next = jnp.sum(residual * residual)
        direction = residual + (norm_next / norm_now) * direction
        norm_now = norm_next
    return coefficients, residual
```

```python
import functools

import jax
import jax.numpy as jnp
from jax import lax
from jax.experimental import pallas as pl
from jax.experimental.pallas import tpu as pltpu
from jax.sharding import PartitionSpec as P

F32 = jnp.float32
BF16 = jnp.bfloat16
RING = 4
CHIPS = RING ** 3
CUTS = ((0, 80), (80, 80), (160, 96))
PLANE = ((1, 0), (3, 0), (0, 1), (0, 3), (1, 1), (1, 3), (3, 1), (3, 3), (2, 0), (0, 2),
         (1, 2), (3, 2), (2, 1), (2, 3), (2, 2))
FAR = 42


def choose(cond, a, b):
    if isinstance(cond, bool):
        return a if cond else b
    return jnp.where(cond, a, b)


def flip(mu, pos):
    out = 0
    for d in (2, 1, 0):
        out = choose(mu[d] == 2, pos[d] // 2, out)
    for d in (2, 1, 0):
        out = choose(mu[d] % 2 == 1, mu[d] // 2, out)
    return out


def turned(k, m1, m2, m3):
    return ((m3, m2, m1), (m2, m1, m3), (m1, m3, m2))[k]


def dim_of(k, role):
    return ((2, 1, 0), (1, 0, 2), (0, 2, 1))[k][role]


def number(mu):
    return mu[0] * 16 + mu[1] * 4 + mu[2]


def parts(s):
    return s // 16, s // 4 % 4, s % 4


def stage(m1, m2, m3):
    return m3 * 16 + m2 * 4 + m1


def children(m1, m2):
    out = []
    if m2 == 0:
        if m1 == 0:
            out += [((1, 0, 0), 0, 1), ((3, 0, 0), 0, -1)]
        if m1 == 1:
            out += [((2, 0, 0), 0, 1)]
        out += [((m1, 1, 0), 1, 1), ((m1, 3, 0), 1, -1)]
    if m2 == 1 and m1 % 2 == 0:
        out += [((m1, 2, 0), 1, 1)]
    if m2 == 3 and m1 % 2 == 1:
        out += [((m1, 2, 0), 1, -1)]
    return out + [((m1, m2, 1), 2, 1), ((m1, m2, 3), 2, -1)]


def kernel(pts_hbm, tgt, ridge, coef_out, res_out, pts, blocks, tl, t_all, w_all, c_all, qs1, qr1, qs2, qr2,
           r_a, r_b, kt, ka, kb, sem_in, ps, pr, ls, lr, bs, br, ts, tr, ws, wr, cs, cr, q1s, q1r, q2s, q2r):
    me = lax.axis_index("pts")
    local = tgt.shape[1]
    dim = pts.shape[1]
    half = local // 2
    wide = 2 * dim
    core = lax.rem(me, 2)
    chip = me // 2
    pos = (chip // 16, lax.rem(chip // 4, 4), lax.rem(chip, 4))

    def shifted(mu, sign=1):
        return tuple(lax.rem(p + 4 + sign * m, 4) for p, m in zip(pos, mu))

    def device(at, c):
        return number(at) * 2 + lax.rem(c, 2)

    partner = device(pos, core + 1)
    load = pltpu.make_async_copy(pts_hbm, pts, sem_in)
    load.start()
    barrier = pltpu.get_barrier_semaphore()
    near = [partner]
    for d in range(3):
        for sign in (1, -1):
            at = shifted(tuple(int(d == i) for i in range(3)), sign)
            near += [device(at, core), device(at, core + 1)]
    for dev in near:
        pl.semaphore_signal(barrier, inc=1, device_id=(dev,), device_id_type=pl.DeviceIdType.MESH)

    target = tgt[...]
    t_all[0, 0] = target
    low = target.astype(BF16)
    rows2 = jnp.concatenate([low[:, :half].astype(F32), low[:, half:].astype(F32)], axis=0).astype(BF16)
    for k in range(3):
        tl[0, k] = rows2
    qs1[...] = jnp.zeros_like(qs1)
    qs2[...] = jnp.zeros_like(qs2)

    load.wait()
    own = pts[...].astype(F32)
    blocks[0] = jnp.concatenate([own[:half], own[half:]], axis=1).astype(BF16)

    def send(src, dst, ssem, rsem, dev):
        return pltpu.make_async_remote_copy(
            src_ref=src, dst_ref=dst, send_sem=ssem, recv_sem=rsem,
            device_id=(dev,), device_id_type=pl.DeviceIdType.MESH)

    def piece(k, src, to, dev):
        cut = pl.ds(*CUTS[k])
        return (send(blocks.at[src, cut], blocks.at[to, cut], ps.at[k, to], pr.at[k, to], dev),
                send(tl.at[src, k], tl.at[to, k], ls.at[k, to], lr.at[k, to], dev))

    def relay(k, m, to, role, sign):
        d = dim_of(k, role)
        step = tuple(sign if i == d else 0 for i in range(3))
        at = tuple(lax.rem(p + 4 + s, 4) for p, s in zip(pos, step))
        c = core + flip(turned(k, *m), pos) + flip(turned(k, *to), at)
        for copy in piece(k, stage(*m), stage(*to), device(at, c)):
            copy.start()

    def arrive(s):
        for k in range(3):
            for copy in piece(k, 0, s, partner):
                copy.wait_recv()

    def send_on(m1, m2):
        for to, role, sign in children(m1, m2):
            for k in range(3):
                relay(k, (m1, m2, 0), to, role, sign)

    pl.semaphore_wait(barrier, len(near))
    pair = (send(blocks.at[0], blocks.at[CHIPS], bs.at[0], br.at[0], partner),
            send(tl.at[0], tl.at[CHIPS], bs.at[1], br.at[1], partner))
    for copy in pair:
        copy.start()
    send_on(0, 0)

    own_t = own.T
    s_row = jnp.sum(own_t * own_t, axis=0, keepdims=True) * (-1.0 / dim)
    s_hi = s_row.astype(BF16).astype(F32)
    s_mid = (s_row - s_hi).astype(BF16).astype(F32)
    s_lo = s_row - s_hi - s_mid
    rows = lax.broadcasted_iota(jnp.int32, (dim, local), 0)
    pieces = jnp.where(rows == 0, s_hi, jnp.where(rows == 1, s_mid, jnp.where(rows == 2, s_lo, 0.0)))
    pieces = pieces.astype(BF16)
    scaled = (own_t * (2.0 / dim)).astype(BF16)
    minus = jnp.full((dim, local), -1.0 / dim, BF16)
    r_a[0:dim] = scaled
    r_a[dim:2 * dim] = minus
    r_a[2 * dim:3 * dim] = minus
    r_a[3 * dim:4 * dim] = pieces
    r_b[0:dim] = minus
    r_b[dim:2 * dim] = scaled
    r_b[2 * dim:3 * dim] = pieces
    r_b[3 * dim:4 * dim] = minus

    lanes = lax.broadcasted_iota(jnp.int32, (half, wide), 1)
    first = lanes < dim
    one = jnp.ones((half, wide), BF16)

    def form(s, keep):
        pb = blocks[s]
        f = pb.astype(F32)
        sq = f * f
        hi = sq.astype(BF16)
        lo = (sq - hi.astype(F32)).astype(BF16)
        hi = pltpu.roll(hi.astype(F32), dim, 1).astype(BF16)
        top = jnp.concatenate([jnp.where(first, pb, hi), jnp.where(first, lo, one)], axis=1)
        bot = jnp.concatenate([jnp.where(first, hi, pb), jnp.where(first, one, lo)], axis=1)
        for h, lhs, r in ((0, top, r_a), (1, bot, r_b)):
            e = jnp.dot(lhs, r[...], preferred_element_type=F32)
            k = jnp.exp(e).astype(BF16)
            kt[s, h * half:(h + 1) * half] = k
            keep[h * half:(h + 1) * half] = k

    lane2 = lax.broadcasted_iota(jnp.int32, (2, half), 1)
    lane1 = lax.rem(lax.broadcasted_iota(jnp.int32, (1, local), 1), half)

    def by_piece(lane, a, b, c):
        return jnp.where(lane < CUTS[1][0], a, jnp.where(lane < CUTS[2][0], b, c))

    def across(ks, weight):
        found = []
        for k in ks:
            x = k.astype(F32) * weight
            x = (x[:, :128] + x[:, 128:256]) + (x[:, 256:384] + x[:, 384:])
            found.append(jnp.sum(x.T, axis=0, keepdims=True))
        return jnp.concatenate(found, axis=1)

    def share(qs, m, q):
        for k in range(3):
            slot = number(turned(k, *m))
            keep = (lane1 >= CUTS[k][0]) & (lane1 < CUTS[k][0] + CUTS[k][1])
            qs[slot] = jnp.where(keep, q, qs[slot])

    t_low = low.astype(F32)

    def absorb(s, m, held, acc):
        ks = [held[0:half], held[half:]]
        v2 = by_piece(lane2, *(tl[s, k].astype(F32) for k in range(3))).astype(BF16)
        acc = tuple(a + jnp.dot(v2, k, preferred_element_type=F32) for a, k in zip(acc, ks))
        if m is not None:
            share(qs1, m, across(ks, t_low))
        return acc

    zero = jnp.zeros((2, local), F32)
    acc = (zero, zero)
    form(0, ka)
    for copy in pair:
        copy.wait_recv()
    acc = absorb(0, None, ka, acc)
    form(CHIPS, kb)
    here = (CHIPS, None, kb, ka)
    for m1, m2 in PLANE:
        s = stage(m1, m2, 0)
        arrive(s)
        send_on(m1, m2)
        acc = absorb(*here[:3], acc)
        form(s, here[3])
        here = (s, (m1, m2, 0), here[3], here[2])

    k_old, k_new = here[2], here[3]
    last_m = here[1]

    def digit(v):
        return jnp.where(v < 2, v, 5 - v)

    def stage_b(j, acc):
        def place(i, m3):
            return digit(lax.rem(i, 4)), digit(i // 4), m3

        m1, m2, _ = place(j, 0)
        for m3 in (1, 3):
            arrive(stage(m1, m2, m3))
        odd = lax.rem(m1 + m2, 2)
        m3 = 1 + 2 * odd
        for k in range(3):
            d = dim_of(k, 2)
            at = tuple(lax.rem(pos[i] + (5 - 2 * odd if i == d else 4), 4) for i in range(3))
            to = (m1, m2, 2)
            c = core + flip(turned(k, m1, m2, m3), pos) + flip(turned(k, *to), at)
            for copy in piece(k, stage(m1, m2, m3), stage(*to), device(at, c)):
                copy.start()
        p1, p2, p3 = place(j - 1, 3)
        before = tuple(jnp.where(j == 0, a, b) for a, b in zip(last_m, (p1, p2, p3)))
        acc = absorb(stage(*before), before, k_old, acc)
        form(stage(m1, m2, 1), k_new)
        acc = absorb(stage(m1, m2, 1), (m1, m2, 1), k_new, acc)
        form(stage(m1, m2, 3), k_old)
        return acc

    acc = lax.fori_loop(0, 16, stage_b, acc)

    def spread(buf, ssem, rsem, p, e):
        mu = parts(e)
        return send(buf.at[0, 0], buf.at[p, e], ssem.at[p, e], rsem.at[p, e], device(shifted(mu), core + p))

    spread(t_all, ts, tr, 1, 0).start()

    @pl.loop(1, CHIPS)
    def _(e):
        @pl.when(e != FAR)
        def _():
            for p in (0, 1):
                spread(t_all, ts, tr, p, e).start()

    def stage_c(j, acc):
        def place(i):
            return digit(lax.rem(i, 4)), digit(i // 4)

        m1, m2 = place(2 * j)
        n1, n2 = place(2 * j + 1)
        arrive(stage(m1, m2, 2))
        arrive(stage(n1, n2, 2))
        p1, p2 = place(2 * j - 1)
        before = (jnp.where(j == 0, digit(3), p1), jnp.where(j == 0, digit(3), p2), jnp.where(j == 0, 3, 2))
        acc = absorb(stage(*before), before, k_old, acc)
        form(stage(m1, m2, 2), k_new)
        acc = absorb(stage(m1, m2, 2), (m1, m2, 2), k_new, acc)
        form(stage(n1, n2, 2), k_old)
        return acc

    acc = lax.fori_loop(0, 8, stage_c, acc)
    for p in (0, 1):
        spread(t_all, ts, tr, p, FAR).start()
    acc = absorb(stage(2, 2, 2), (2, 2, 2), k_old, acc)

    def q_copy(qs, qr, ssem, rsem, s):
        mu = parts(s)
        return send(qs.at[s], qr.at[s], ssem.at[s], rsem.at[s], device(shifted(mu, -1), core + flip(mu, pos)))

    def others(fn):
        fn(1, 0)

        @pl.loop(1, CHIPS)
        def _(e):
            fn(0, e)
            fn(1, e)

    @pl.loop(1, CHIPS)
    def _(s):
        q_copy(qs1, qr1, q1s, q1r, s).start()

    for copy in pair:
        copy.wait_send()

    @pl.loop(1, CHIPS)
    def _(s):
        for k in range(3):
            for copy in piece(k, 0, s, partner):
                copy.wait_send()

    others(lambda p, e: spread(t_all, ts, tr, p, e).wait_recv())
    others(lambda p, e: spread(t_all, ts, tr, p, e).wait_send())
    t_whole = t_all[...]
    norm0 = jnp.sum(t_whole * t_whole)
    weight = ridge[0, 0]
    base = acc[0][0:1] + acc[1][1:2] + weight * target

    @pl.loop(1, CHIPS)
    def _(s):
        q_copy(qs1, qr1, q1s, q1r, s).wait_recv()

    w_all[0, 0] = base + jnp.sum(qr1[1:CHIPS], axis=0)
    others(lambda p, e: spread(w_all, ws, wr, p, e).start())

    @pl.loop(1, CHIPS)
    def _(s):
        q_copy(qs1, qr1, q1s, q1r, s).wait_send()

    others(lambda p, e: spread(w_all, ws, wr, p, e).wait_recv())
    others(lambda p, e: spread(w_all, ws, wr, p, e).wait_send())

    w_whole = w_all[...]
    step0 = norm0 / jnp.sum(t_whole * w_whole)
    r1 = t_whole - step0 * w_whole
    norm1 = jnp.sum(r1 * r1)
    t_all[...] = r1 + (norm1 / norm0) * t_whole

    d_own = t_all[0, 0]
    d_low = d_own.astype(BF16).astype(F32)

    def again(s, v, acc):
        ks = [kt[s, 0:half], kt[s, half:]]
        vb = v.astype(BF16)
        for h in (0, 1):
            acc = acc + jnp.dot(vb[:, h * half:(h + 1) * half], ks[h], preferred_element_type=F32)
        return acc, ks

    acc = jnp.zeros((1, local), F32)
    acc, _ = again(0, d_own, acc)
    acc, _ = again(CHIPS, t_all[1, 0], acc)

    def second(s, carry):
        acc, curve = carry
        m3, m2, m1 = parts(s)
        found = []
        for k in range(3):
            mu = turned(k, m1, m2, m3)
            found.append(t_all[flip(mu, pos), number(mu)])
        v = by_piece(lane1, *found)
        acc, ks = again(s, v, acc)
        q = across(ks, d_low)
        share(qs2, (m1, m2, m3), q)
        return acc, curve + q * v

    def two(i, carry):
        return second(2 * i + 1, second(2 * i, carry))

    carry = second(1, (acc, jnp.zeros((1, local), F32)))
    acc, curve = lax.fori_loop(1, CHIPS // 2, two, carry)
    applied = acc + weight * d_own
    part = jnp.sum(d_own * applied) + jnp.sum(curve)
    c_all[0, 0] = jnp.full((1, 128), part, F32)

    others(lambda p, e: spread(c_all, cs, cr, p, e).start())

    @pl.loop(1, CHIPS)
    def _(s):
        q_copy(qs2, qr2, q2s, q2r, s).start()

    others(lambda p, e: spread(c_all, cs, cr, p, e).wait_recv())
    others(lambda p, e: spread(c_all, cs, cr, p, e).wait_send())

    @pl.loop(1, CHIPS)
    def _(s):
        q_copy(qs2, qr2, q2s, q2r, s).wait()

    applied = applied + jnp.sum(qr2[1:CHIPS], axis=0)
    curvature = jnp.sum(jnp.sum(c_all[...], axis=(0, 1)), axis=0, keepdims=True)[:, 0:1]
    step1 = norm1 / curvature
    coef_out[...] = step0 * target + step1 * d_own
    res_out[...] = target - step0 * w_all[0, 0] - step1 * applied


def body(points, targets, ridge_weight):
    local, dim = points.shape
    half = local // 2
    dma = pltpu.SemaphoreType.DMA
    vec = jax.ShapeDtypeStruct((1, local), F32)
    rows = pltpu.VMEM((CHIPS, 1, local), F32)
    both = pltpu.VMEM((2, CHIPS, 1, local), F32)
    coef, res = pl.pallas_call(
        kernel,
        out_shape=(vec, vec),
        in_specs=[
            pl.BlockSpec(memory_space=pl.ANY),
            pl.BlockSpec(memory_space=pltpu.VMEM),
            pl.BlockSpec(memory_space=pltpu.SMEM),
        ],
        out_specs=(pl.BlockSpec(memory_space=pltpu.VMEM), pl.BlockSpec(memory_space=pltpu.VMEM)),
        scratch_shapes=[
            pltpu.VMEM((local, dim), BF16),
            pltpu.VMEM((CHIPS + 1, half, 2 * dim), BF16),
            pltpu.VMEM((CHIPS + 1, 3, 2, half), BF16),
            both, both,
            pltpu.VMEM((2, CHIPS, 1, 128), F32),
            rows, rows, rows, rows,
            pltpu.VMEM((4 * dim, local), BF16),
            pltpu.VMEM((4 * dim, local), BF16),
            pltpu.VMEM((CHIPS + 1, local, local), BF16),
            pltpu.VMEM((local, local), BF16),
            pltpu.VMEM((local, local), BF16),
            dma,
            dma((3, CHIPS)), dma((3, CHIPS)),
            dma((3, CHIPS)), dma((3, CHIPS)),
            dma((2,)), dma((2,)),
            dma((2, CHIPS)), dma((2, CHIPS)),
            dma((2, CHIPS)), dma((2, CHIPS)),
            dma((2, CHIPS)), dma((2, CHIPS)),
            dma((CHIPS,)), dma((CHIPS,)),
            dma((CHIPS,)), dma((CHIPS,)),
        ],
        compiler_params=pltpu.CompilerParams(
            collective_id=0, has_side_effects=True, vmem_limit_bytes=62 * 1024 * 1024),
    )(points, targets.reshape(1, local), ridge_weight.reshape(1, 1))
    return coef.reshape(local), res.reshape(local)


def solution(mesh):
    return jax.shard_map(
        body, mesh=mesh,
        in_specs=(P("pts", None), P("pts"), P()),
        out_specs=(P("pts"), P("pts")), check_vma=False)
```

```python
import functools

import jax
import jax.numpy as jnp
from jax import lax
from jax.experimental import pallas as pl
from jax.experimental.pallas import tpu as pltpu
from jax.sharding import PartitionSpec as P

F32 = jnp.float32
BF16 = jnp.bfloat16
RING = 4
CHIPS = RING ** 3
CUTS = ((0, 80), (80, 80), (160, 96))


def reach(m):
    return sum(min(v, RING - v) for v in m)


def ordered():
    every = [(a, b, c) for c in range(RING) for b in range(RING) for a in range(RING) if (a, b, c) != (0, 0, 0)]
    late = (0.0, 0.6, 1.2, 0.6)
    return sorted(every, key=lambda m: (reach(m) + late[m[2]], m[2], m[1] % 2, m[0] % 2, m))


ORDER = [m[2] * 16 + m[1] * 4 + m[0] for m in ordered()]
WORDS = [sum(v * 64 ** n for n, v in enumerate(ORDER[i:i + 5])) for i in range(0, len(ORDER), 5)]


def place(i):
    word = WORDS[-1]
    for n in reversed(range(len(WORDS) - 1)):
        word = jnp.where(i // 5 == n, WORDS[n], word)
    at = lax.rem(i, 5)
    code = word // 64 ** 4
    for n in reversed(range(4)):
        code = jnp.where(at == n, word // 64 ** n % 64, code)
    return code


def choose(cond, a, b):
    if isinstance(cond, bool):
        return a if cond else b
    return jnp.where(cond, a, b)


def flip(mu, pos):
    out = 0
    for d in (2, 1, 0):
        out = choose(mu[d] == 2, pos[d] // 2, out)
    for d in (2, 1, 0):
        out = choose(mu[d] % 2 == 1, mu[d] // 2, out)
    return out


def turned(k, m1, m2, m3):
    return ((m3, m2, m1), (m2, m1, m3), (m1, m3, m2))[k]


def dim_of(k, role):
    return ((2, 1, 0), (1, 0, 2), (0, 2, 1))[k][role]


def number(mu):
    return mu[0] * 16 + mu[1] * 4 + mu[2]


def parts(s):
    return s // 16, s // 4 % 4, s % 4


def far(v):
    return choose(v == 0, 2, choose(v == 3, 0, choose(v == 2, 3, 1)))


def stage(m1, m2, m3):
    return m3 * 16 + m2 * 4 + m1


def kernel(pts_hbm, tgt, ridge, coef_out, res_out, pts, blocks, tl, t_all, w_all, c_all, qs1, qr1, qs2, qr2,
           r_a, r_b, kt, ka, kb, sem_in, pr, lr, sems):
    me = lax.axis_index("pts")
    local = tgt.shape[1]
    dim = pts.shape[0]
    half = local // 2
    wide = 2 * dim
    core = lax.rem(me, 2)
    chip = me // 2
    pos = (chip // 16, lax.rem(chip // 4, 4), lax.rem(chip, 4))

    def shifted(mu, sign=1):
        return tuple(lax.rem(p + 4 + sign * m, 4) for p, m in zip(pos, mu))

    def device(at, c):
        return number(at) * 2 + lax.rem(c, 2)

    partner = device(pos, core + 1)
    load = pltpu.make_async_copy(pts_hbm, pts, sem_in)
    load.start()
    barrier = pltpu.get_barrier_semaphore()
    near = [partner]
    for d in range(3):
        for sign in (1, -1):
            at = shifted(tuple(int(d == i) for i in range(3)), sign)
            near += [device(at, core), device(at, core + 1)]
    for dev in near:
        pl.semaphore_signal(barrier, inc=1, device_id=(dev,), device_id_type=pl.DeviceIdType.MESH)

    target = tgt[...]
    t_all[0] = target
    low = target.astype(BF16)
    rows2 = jnp.concatenate([low[:, :half].astype(F32), low[:, half:].astype(F32)], axis=0).astype(BF16)
    for k in range(3):
        tl[0, k] = rows2
    qs1[...] = jnp.zeros_like(qs1)
    qs2[...] = jnp.zeros_like(qs2)

    load.wait()
    own_t = pts[...].astype(F32)
    own = own_t.T
    blocks[0] = jnp.concatenate([own[:half], own[half:]], axis=1).astype(BF16)

    def send(src, dst, ssem, rsem, dev):
        return pltpu.make_async_remote_copy(
            src_ref=src, dst_ref=dst, send_sem=ssem, recv_sem=rsem,
            device_id=(dev,), device_id_type=pl.DeviceIdType.MESH)

    def piece(k, src, to, dev):
        cut = pl.ds(*CUTS[k])
        return (send(blocks.at[src, cut], blocks.at[to, cut], sems.at[0], pr.at[to], dev),
                send(tl.at[src, k], tl.at[to, k], sems.at[1], lr.at[to], dev))

    def relay(m, to, role, sign):
        for k in range(3):
            d = dim_of(k, role)
            at = tuple(lax.rem(p + 4 + sign, 4) if i == d else p for i, p in enumerate(pos))
            c = core + flip(turned(k, *m), pos) + flip(turned(k, *to), at)
            for copy in piece(k, stage(*m), stage(*to), device(at, c)):
                copy.start()

    def arrive(s):
        send(blocks.at[s], blocks.at[s], sems.at[0], pr.at[s], partner).wait_recv()
        send(tl.at[s], tl.at[s], sems.at[1], lr.at[s], partner).wait_recv()

    def send_on(m1, m2, m3):
        m = (m1, m2, m3)

        @pl.when(m3 == 0)
        def _():
            @pl.when((m1 == 1) & (m2 == 0))
            def _():
                relay((1, 0, 0), (2, 0, 0), 0, 1)

            @pl.when(m2 == 0)
            def _():
                relay((m1, 0, 0), (m1, 1, 0), 1, 1)
                relay((m1, 0, 0), (m1, 3, 0), 1, -1)

            even = lax.rem(m1, 2) == 0

            @pl.when(((m2 == 1) & even) | ((m2 == 3) & (lax.rem(m1, 2) == 1)))
            def _():
                relay((m1, m2, 0), (m1, 2, 0), 1, 2 - m2)

            relay((m1, m2, 0), (m1, m2, 1), 2, 1)
            relay((m1, m2, 0), (m1, m2, 3), 2, -1)

        @pl.when(m3 == 1 + 2 * lax.rem(m1 + m2, 2))
        def _():
            relay(m, (m1, m2, 2), 2, 2 - m3)

    pl.semaphore_wait(barrier, len(near))
    pair = (send(blocks.at[0], blocks.at[CHIPS], sems.at[2], sems.at[3], partner),
            send(tl.at[0], tl.at[CHIPS], sems.at[4], sems.at[5], partner))
    for copy in pair:
        copy.start()
    for role in range(3):
        for to, sign in ((1, 1), (3, -1)):
            relay((0, 0, 0), tuple(to if i == role else 0 for i in range(3)), role, sign)
    s_row = jnp.sum(own_t * own_t, axis=0, keepdims=True) * (-1.0 / dim)
    s_hi = s_row.astype(BF16).astype(F32)
    s_mid = (s_row - s_hi).astype(BF16).astype(F32)
    s_lo = s_row - s_hi - s_mid
    rows = lax.broadcasted_iota(jnp.int32, (dim, local), 0)
    pieces = jnp.where(rows == 0, s_hi, jnp.where(rows == 1, s_mid, jnp.where(rows == 2, s_lo, 0.0)))
    pieces = pieces.astype(BF16)
    scaled = (own_t * (2.0 / dim)).astype(BF16)
    minus = jnp.full((dim, local), -1.0 / dim, BF16)
    r_a[0:dim] = scaled
    r_a[dim:2 * dim] = minus
    r_a[2 * dim:3 * dim] = minus
    r_a[3 * dim:4 * dim] = pieces
    r_b[0:dim] = minus
    r_b[dim:2 * dim] = scaled
    r_b[2 * dim:3 * dim] = pieces
    r_b[3 * dim:4 * dim] = minus

    lanes = lax.broadcasted_iota(jnp.int32, (half, wide), 1)
    first = lanes < dim
    one = jnp.ones((half, wide), BF16)

    def form(s, keep):
        pb = blocks[s]
        f = pb.astype(F32)
        sq = f * f
        hi = sq.astype(BF16)
        lo = (sq - hi.astype(F32)).astype(BF16)
        hi = pltpu.roll(hi.astype(F32), dim, 1).astype(BF16)
        top = jnp.concatenate([jnp.where(first, pb, hi), jnp.where(first, lo, one)], axis=1)
        bot = jnp.concatenate([jnp.where(first, hi, pb), jnp.where(first, one, lo)], axis=1)
        for h, lhs, r in ((0, top, r_a), (1, bot, r_b)):
            e = jnp.dot(lhs, r[...], preferred_element_type=F32)
            k = jnp.exp(e).astype(BF16)
            kt[s, h * half:(h + 1) * half] = k
            keep[h * half:(h + 1) * half] = k

    lane2 = lax.broadcasted_iota(jnp.int32, (2, half), 1)
    lane1 = lax.rem(lax.broadcasted_iota(jnp.int32, (1, local), 1), half)

    def by_piece(lane, a, b, c):
        return jnp.where(lane < CUTS[1][0], a, jnp.where(lane < CUTS[2][0], b, c))

    def across(ks, weight):
        found = []
        for k in ks:
            x = k.astype(F32) * weight
            x = (x[:, :128] + x[:, 128:256]) + (x[:, 256:384] + x[:, 384:])
            found.append(jnp.sum(x.T, axis=0, keepdims=True))
        return jnp.concatenate(found, axis=1)

    def share(qs, m, q):
        for k in range(3):
            slot = number(turned(k, *m))
            keep = (lane1 >= CUTS[k][0]) & (lane1 < CUTS[k][0] + CUTS[k][1])
            qs[slot] = jnp.where(keep, q, qs[slot])

    t_low = low.astype(F32)

    def absorb(s, m, held, acc):
        ks = [held[0:half], held[half:]]
        v2 = by_piece(lane2, *(tl[s, k].astype(F32) for k in range(3))).astype(BF16)
        acc = tuple(a + jnp.dot(v2, k, preferred_element_type=F32) for a, k in zip(acc, ks))
        if m is not None:
            share(qs1, m, across(ks, t_low))
        return acc

    zero = jnp.zeros((2, local), F32)
    acc = (zero, zero)
    form(0, ka)
    for copy in pair:
        copy.wait_recv()
    acc = absorb(0, None, ka, acc)
    form(CHIPS, kb)

    def spread(buf, sem, p, e):
        mu = parts(e)
        return send(buf.at[0], buf.at[p * CHIPS + e], sems.at[sem], sems.at[sem + 1], device(shifted(mu), core + p))

    def gathered(buf, sem):
        rest = buf.at[pl.ds(1, buf.shape[0] - 1)]
        return send(rest, rest, sems.at[sem], sems.at[sem + 1], partner)

    def digits(code):
        m3, m2, m1 = parts(code)
        return m1, m2, m3

    def come(code):
        arrive(code)
        send_on(*digits(code))

    def greet(code):
        mu = turned(0, *digits(code))
        back = number(tuple(lax.rem(4 - v, 4) for v in mu))
        for p in (0, 1):
            spread(t_all, 6, p, back).start()

    spread(t_all, 6, 1, 0).start()

    def two(i, acc):
        a, b = place(2 * i), place(2 * i + 1)
        before = jnp.where(i == 0, 0, place(2 * i - 1))
        come(a)
        come(b)
        acc = absorb(jnp.where(i == 0, CHIPS, before), digits(before), kb, acc)
        form(a, ka)
        greet(a)
        acc = absorb(a, digits(a), ka, acc)
        form(b, kb)
        greet(b)
        return acc

    acc = lax.fori_loop(0, 31, two, acc)
    code = ORDER[62]
    come(code)
    acc = absorb(ORDER[61], digits(ORDER[61]), kb, acc)
    form(code, ka)
    greet(code)
    acc = absorb(code, digits(code), ka, acc)

    def q_copy(qs, qr, sem, s):
        mu = parts(s)
        return send(qs.at[s], qr.at[s], sems.at[sem], sems.at[sem + 1], device(shifted(mu, -1), core + flip(mu, pos)))

    def farthest_first(fn):
        @pl.loop(0, CHIPS - 1)
        def _(i):
            fn(far(i // 16) * 16 + far(i // 4 % 4) * 4 + far(i % 4))

    farthest_first(lambda e: q_copy(qs1, qr1, 8, e).start())
    for copy in pair:
        copy.wait_send()
    gathered(blocks.at[pl.ds(0, CHIPS)], 0).wait_send()
    gathered(tl.at[pl.ds(0, CHIPS)], 1).wait_send()
    gathered(t_all, 6).wait()
    t_whole = t_all[...]
    norm0 = jnp.sum(t_whole * t_whole)
    weight = ridge[0, 0]
    base = acc[0][0:1] + acc[1][1:2] + weight * target
    send(qs1.at[pl.ds(1, CHIPS - 1)], qr1.at[pl.ds(1, CHIPS - 1)], sems.at[8], sems.at[9], partner).wait_recv()
    w_all[0] = base + jnp.sum(qr1[1:CHIPS], axis=0)

    def to_both(buf, sem):
        def both(e):
            for p in (0, 1):
                spread(buf, sem, p, e).start()

        farthest_first(both)
        spread(buf, sem, 1, 0).start()

    to_both(w_all, 10)
    send(qs1.at[pl.ds(1, CHIPS - 1)], qr1.at[pl.ds(1, CHIPS - 1)], sems.at[8], sems.at[9], partner).wait_send()
    gathered(w_all, 10).wait()
    w_whole = w_all[...]
    step0 = norm0 / jnp.sum(t_whole * w_whole)
    r1 = t_whole - step0 * w_whole
    norm1 = jnp.sum(r1 * r1)
    t_all[...] = r1 + (norm1 / norm0) * t_whole

    d_own = t_all[0]
    d_low = d_own.astype(BF16).astype(F32)

    def again(s, v, acc):
        ks = [kt[s, 0:half], kt[s, half:]]
        vb = v.astype(BF16)
        for h in (0, 1):
            acc = acc + jnp.dot(vb[:, h * half:(h + 1) * half], ks[h], preferred_element_type=F32)
        return acc, ks

    acc = jnp.zeros((1, local), F32)
    acc, _ = again(0, d_own, acc)
    acc, _ = again(CHIPS, t_all[CHIPS], acc)

    def second(s, carry):
        acc, curve = carry
        m3, m2, m1 = parts(s)
        found = []
        for k in range(3):
            mu = turned(k, m1, m2, m3)
            found.append(t_all[flip(mu, pos) * CHIPS + number(mu)])
        v = by_piece(lane1, *found)
        acc, ks = again(s, v, acc)
        q = across(ks, d_low)
        share(qs2, (m1, m2, m3), q)
        return acc, curve + q * v

    def next_two(i, carry):
        return second(2 * i + 1, second(2 * i, carry))

    carry = second(1, (acc, jnp.zeros((1, local), F32)))
    acc, curve = lax.fori_loop(1, CHIPS // 2, next_two, carry)
    applied = acc + weight * d_own
    part = jnp.sum(d_own * applied) + jnp.sum(curve)
    c_all[0] = jnp.full((1, 128), part, F32)
    to_both(c_all, 12)
    farthest_first(lambda e: q_copy(qs2, qr2, 14, e).start())
    gathered(c_all, 12).wait()
    send(qs2.at[pl.ds(1, CHIPS - 1)], qr2.at[pl.ds(1, CHIPS - 1)], sems.at[14], sems.at[15], partner).wait()
    applied = applied + jnp.sum(qr2[1:CHIPS], axis=0)
    curvature = jnp.sum(c_all[...], axis=0)[:, 0:1]
    step1 = norm1 / curvature
    coef_out[...] = step0 * target + step1 * d_own
    res_out[...] = target - step0 * w_all[0] - step1 * applied


def body(points, targets, ridge_weight):
    local, dim = points.shape
    half = local // 2
    dma = pltpu.SemaphoreType.DMA
    vec = jax.ShapeDtypeStruct((1, local), F32)
    rows = pltpu.VMEM((CHIPS, 1, local), F32)
    both = pltpu.VMEM((2 * CHIPS, 1, local), F32)
    coef, res = pl.pallas_call(
        kernel,
        out_shape=(vec, vec),
        in_specs=[
            pl.BlockSpec(memory_space=pl.ANY),
            pl.BlockSpec(memory_space=pltpu.VMEM),
            pl.BlockSpec(memory_space=pltpu.SMEM),
        ],
        out_specs=(pl.BlockSpec(memory_space=pltpu.VMEM), pl.BlockSpec(memory_space=pltpu.VMEM)),
        scratch_shapes=[
            pltpu.VMEM((dim, local), BF16),
            pltpu.VMEM((CHIPS + 1, half, 2 * dim), BF16),
            pltpu.VMEM((CHIPS + 1, 3, 2, half), BF16),
            both, both,
            pltpu.VMEM((2 * CHIPS, 1, 128), F32),
            rows, rows, rows, rows,
            pltpu.VMEM((4 * dim, local), BF16),
            pltpu.VMEM((4 * dim, local), BF16),
            pltpu.VMEM((CHIPS + 1, local, local), BF16),
            pltpu.VMEM((local, local), BF16),
            pltpu.VMEM((local, local), BF16),
            dma, dma((CHIPS,)), dma((CHIPS,)), dma((16,)),
        ],
        compiler_params=pltpu.CompilerParams(
            collective_id=0, has_side_effects=True, vmem_limit_bytes=62 * 1024 * 1024),
    )(points.T, targets.reshape(1, local), ridge_weight.reshape(1, 1))
    return coef.reshape(local), res.reshape(local)


def solution(mesh):
    return jax.shard_map(
        body, mesh=mesh,
        in_specs=(P("pts", None), P("pts"), P()),
        out_specs=(P("pts"), P("pts")), check_vma=False)
```

```python
import jax
import jax.numpy as jnp
from jax import lax
from jax.experimental import pallas as pl
from jax.experimental.pallas import tpu as pltpu
from jax.sharding import PartitionSpec as P

F32 = jnp.float32
BF16 = jnp.bfloat16
TREE = (
    ((0, 0, 1), 0, 2, 1), ((0, 1, 0), 0, 1, 1), ((1, 0, 0), 0, 0, 1), ((1, 3, 0), 3, 1, -1), ((1, 1, 0), 2, 0, 1),
    ((3, 0, 1), 1, 0, -1), ((0, 1, 1), 1, 1, 1), ((0, 1, 3), 2, 2, -1), ((1, 0, 1), 3, 2, 1), ((0, 1, 2), 8, 2, -1),
    ((3, 0, 2), 6, 2, 1), ((1, 1, 1), 5, 2, 1), ((1, 2, 0), 4, 1, -1), ((1, 3, 3), 4, 2, -1), ((2, 0, 1), 6, 0, -1),
    ((2, 3, 0), 4, 0, 1), ((0, 2, 1), 7, 1, 1), ((1, 1, 3), 5, 2, -1), ((1, 3, 1), 9, 1, -1), ((1, 2, 1), 12, 1, 1),
    ((1, 2, 3), 13, 2, -1), ((3, 1, 2), 10, 0, -1), ((2, 3, 1), 15, 1, -1), ((2, 3, 3), 14, 0, 1), ((3, 3, 2), 11, 1, -1),
    ((2, 2, 1), 20, 0, 1), ((1, 2, 2), 21, 2, -1), ((2, 1, 2), 22, 0, -1), ((0, 0, 2), 1, 2, 1), ((0, 2, 0), 2, 1, 1),
    ((2, 0, 0), 3, 0, 1), ((0, 2, 2), 10, 1, 1), ((2, 0, 2), 11, 0, -1), ((2, 2, 0), 16, 1, -1), ((2, 2, 2), 26, 2, 1))
PLACES = ((0, 0, 0),) + tuple(t[0] for t in TREE)
SLOTS = len(PLACES)
SELF = 29
UNITS = 2 * SELF + SLOTS - SELF
CHUNKS = ((1, 3), (4, 6), (10, 10), (20, 6), (26, 3), (SELF, SLOTS - SELF))
ALL = tuple((z, y, x) for z in range(4) for y in range(4) for x in range(4))


def chunk_of(s):
    return [lo <= s < lo + n for lo, n in CHUNKS].index(True)


def hops(m):
    return sum(min(v, 4 - v) for v in m)


def slot_of(u):
    return (u // 2, u % 2) if u < 2 * SELF else (u - SELF, None)


FAR_UNITS = sorted(range(2, UNITS), key=lambda u: -hops(PLACES[slot_of(u)[0]]))
FAR_CHIPS = sorted(ALL, key=lambda m: -hops(m))


def kernel(pts_hbm, tgt, ridge, coef_out, res_out, pts, bl, tl, tu, rr, qs1, qr1, qs2, qr2, ca, cb, cc,
           r_a, r_b, kt, ka, kb, sem_in, gb, gt, db, dt, sems, ack):
    me = lax.axis_index("pts")
    local = tgt.shape[1]
    dim = pts.shape[0]
    half = local // 2
    wide = 2 * dim
    core = lax.rem(me, 2)
    chip = me // 2
    pos = (chip // 16, lax.rem(chip // 4, 4), lax.rem(chip, 4))
    axis = [[lax.rem(pos[d] + a, 4) * (32, 8, 2)[d] for a in range(4)] for d in range(3)]
    cores = (core, 1 - core)
    upper = [p // 2 for p in pos]

    def device(m, c, sign=1):
        return sum(axis[d][sign * m[d] % 4] for d in range(3)) + c

    def split(s):
        return upper[PLACES[s].index(2)]

    partner = device((0, 0, 0), cores[1])
    load = pltpu.make_async_copy(pts_hbm, pts, sem_in)
    load.start()
    barrier = pltpu.get_barrier_semaphore()
    near = [partner] + [device(tuple(int(d == i) for i in range(3)), core, sign) for d in range(3) for sign in (1, -1)]
    for dev in near:
        pl.semaphore_signal(barrier, inc=1, device_id=(dev,), device_id_type=pl.DeviceIdType.MESH)

    target = tgt[...]
    tl[0, 0] = target
    tu[0] = target
    t_low = target.astype(BF16).astype(F32)

    load.wait()
    own_t = pts[...].astype(F32)
    own = own_t.T
    bl[0, 0] = jnp.concatenate([own[:half], own[half:]], axis=1).astype(BF16)

    def send(src, dst, ssem, rsem, dev):
        return pltpu.make_async_remote_copy(
            src_ref=src, dst_ref=dst, send_sem=ssem, recv_sem=rsem,
            device_id=(dev,), device_id_type=pl.DeviceIdType.MESH)

    def hop(s):
        _, src, d, sign = TREE[s - 1]
        g = chunk_of(s)
        dev = device(tuple(int(d == i) for i in range(3)), core, sign)
        return (send(bl.at[0, src], bl.at[0, s], sems.at[0], gb.at[g], dev),
                send(tl.at[0, src], tl.at[0, s], sems.at[1], gt.at[g], dev))

    def across_chip(s):
        g = chunk_of(s) if s else len(CHUNKS)
        return (send(bl.at[0, s], bl.at[1, s], sems.at[2], db.at[g], partner),
                send(tl.at[0, s], tl.at[1, s], sems.at[3], dt.at[g], partner))

    def start(copies):
        for copy in copies:
            copy.start()

    def arrive(plane, g):
        lo, n = CHUNKS[g] if g < len(CHUNKS) else (0, 1)
        for buf, sem in ((bl, (gb, db)[plane]), (tl, (gt, dt)[plane])):
            ref = buf.at[plane, pl.ds(lo, n)]
            send(ref, ref, sems.at[0], sem.at[g], partner).wait_recv()

    def serve(g):
        arrive(0, g)
        lo, n = CHUNKS[g]
        for s in range(1, SLOTS):
            if lo <= TREE[s - 1][1] < lo + n:
                start(hop(s))
        for s in range(lo, lo + n):
            start(across_chip(s))
        for s in range(lo, lo + n):
            pl.semaphore_signal(ack, inc=1, device_id=(device(PLACES[s], core, -1),), device_id_type=pl.DeviceIdType.MESH)

    def whole(buf, lo, sem):
        rest = buf.at[pl.ds(lo, buf.shape[0] - lo)]
        return send(rest, rest, sems.at[sem], sems.at[sem + 1], partner)

    def to_owner(qs, qr, sem, u):
        s, plane = slot_of(u)
        c = cores[plane] if plane is not None else lax.rem(core + split(s), 2)
        return send(qs.at[u], qr.at[u], sems.at[sem], sems.at[sem + 1], device(PLACES[s], c, -1))

    def to_user(buf, sem, u):
        s, plane = slot_of(u)
        c = cores[plane] if plane is not None else lax.rem(core + 1 + split(s), 2)
        return send(buf.at[0], buf.at[u], sems.at[sem], sems.at[sem + 1], device(PLACES[s], c))

    def to_all(buf, sem):
        for m in FAR_CHIPS:
            for p in (0, 1):
                if hops(m) + p:
                    at = p * 64 + m[0] * 16 + m[1] * 4 + m[2]
                    send(buf.at[0], buf.at[at], sems.at[sem], sems.at[sem + 1], device(m, cores[p])).start()

    pl.semaphore_wait(barrier, len(near))
    for s in range(1, SLOTS):
        if TREE[s - 1][1] == 0:
            start(hop(s))
    start(across_chip(0))

    s_row = jnp.sum(own_t * own_t, axis=0, keepdims=True) * (-1.0 / dim)
    s_hi = s_row.astype(BF16).astype(F32)
    s_mid = (s_row - s_hi).astype(BF16).astype(F32)
    s_lo = s_row - s_hi - s_mid
    rows = lax.broadcasted_iota(jnp.int32, (dim, local), 0)
    pieces = jnp.where(rows == 0, s_hi, jnp.where(rows == 1, s_mid, jnp.where(rows == 2, s_lo, 0.0)))
    pieces = pieces.astype(BF16)
    scaled = (own_t * (2.0 / dim)).astype(BF16)
    minus = jnp.full((dim, local), -1.0 / dim, BF16)
    r_a[0:dim] = scaled
    r_a[dim:2 * dim] = minus
    r_a[2 * dim:3 * dim] = minus
    r_a[3 * dim:4 * dim] = pieces
    r_b[0:dim] = minus
    r_b[dim:2 * dim] = scaled
    r_b[2 * dim:3 * dim] = pieces
    r_b[3 * dim:4 * dim] = minus

    lanes = lax.broadcasted_iota(jnp.int32, (half, wide), 1)
    first = lanes < dim
    one = jnp.ones((half, wide), BF16)

    def form(u, plane, s, keep):
        if not (isinstance(u, int) and u == 0):
            tu[u] = tl[plane, s]
        pb = bl[plane, s]
        f = pb.astype(F32)
        sq = f * f
        hi = sq.astype(BF16)
        lo = (sq - hi.astype(F32)).astype(BF16)
        hi = pltpu.roll(hi.astype(F32), dim, 1).astype(BF16)
        top = jnp.concatenate([jnp.where(first, pb, hi), jnp.where(first, lo, one)], axis=1)
        bot = jnp.concatenate([jnp.where(first, hi, pb), jnp.where(first, one, lo)], axis=1)
        for h, lhs, r in ((0, top, r_a), (1, bot, r_b)):
            e = jnp.dot(lhs, r[...], preferred_element_type=F32)
            k = jnp.exp(e).astype(BF16)
            kt[u, h * half:(h + 1) * half] = k
            keep[h * half:(h + 1) * half] = k

    def across(ks, weight):
        found = []
        for k in ks:
            x = k.astype(F32) * weight
            x = (x[:, :128] + x[:, 128:256]) + (x[:, 256:384] + x[:, 384:])
            found.append(jnp.sum(x.T, axis=0, keepdims=True))
        return jnp.concatenate(found, axis=1)

    def down(ks, v, acc):
        vb = v.astype(BF16)
        for h in (0, 1):
            acc = acc + jnp.dot(vb[:, h * half:(h + 1) * half], ks[h], preferred_element_type=F32)
        return acc

    def absorb(u, held, carry, factor=None):
        acc, tw = carry
        ks = [held[0:half], held[half:]]
        v = tu[u]
        q = across(ks, t_low)
        qs1[u] = q
        part = q * v
        if factor is not None:
            part = part * factor
        return down(ks, v, acc), tw + part

    zero = jnp.zeros((1, local), F32)
    form(0, 0, 0, ka)
    acc = down([ka[0:half], ka[half:]], target, zero)
    arrive(1, len(CHUNKS))
    form(1, 1, 0, kb)
    carry = (acc, zero)
    sent, ready = [], []

    def send_ready():
        for u in ready:
            to_owner(qs1, qr1, 8, u).start()
        sent.extend(ready)
        ready.clear()

    last = 1
    for g, (lo, n) in enumerate(CHUNKS):
        serve(g)
        send_ready()
        own_only = lo == SELF
        if own_only:
            arrive(1, g)

        def unit(f, lo=lo, n=n, own_only=own_only):
            if own_only:
                s = lo + f
                plane = split(lo)
                for i in range(1, n):
                    plane = jnp.where(f == i, split(lo + i), plane)
                return s + SELF, plane, s
            plane = jnp.where(f < n, 0, 1)
            s = lo + f - plane * n
            return 2 * s + plane, plane, s

        def two(i, carry, g=g, n=n, unit=unit, own_only=own_only, last=last):
            if not own_only:
                @pl.when(i == n // 2)
                def _():
                    arrive(1, g)

            a, b = unit(2 * i), unit(2 * i + 1)
            before = jnp.where(i == 0, last, unit(2 * i - 1)[0])
            factor = jnp.where(i == 0, 0.0, 1.0) if last == 1 else None
            carry = absorb(before, kb, carry, factor)
            form(*a, ka)
            carry = absorb(a[0], ka, carry)
            form(*b, kb)
            return carry

        carry = lax.fori_loop(0, n // 2 if own_only else n, two, carry)
        if last > 1:
            ready.append(last)
        if own_only:
            carry = absorb(lo + n - 2 + SELF, kb, carry)
            form(UNITS - 1, split(SLOTS - 1), SLOTS - 1, ka)
            carry = absorb(UNITS - 1, ka, carry)
            ready.extend(range(2 * SELF, UNITS))
        else:
            last = 2 * (lo + n - 1) + 1
            ready.extend(u for u in range(2 * lo, 2 * (lo + n)) if u != last)

    ready.reverse()
    send_ready()
    acc, tw = carry
    weight = ridge[0, 0]
    base = acc + weight * target
    lane = lax.broadcasted_iota(jnp.int32, (1, 128), 1)
    ca[0] = jnp.where(lane == 0, jnp.sum(tw + target * base), jnp.where(lane == 1, jnp.sum(target * target), 0.0))
    pl.semaphore_wait(ack, SLOTS - 1)
    to_all(ca, 6)
    moved = bl.at[0, pl.ds(1, SLOTS - 1)], tl.at[0, pl.ds(1, SLOTS - 1)], bl.at[0], tl.at[0]
    for i, ref in enumerate(moved):
        send(ref, ref, sems.at[i], sem_in, partner).wait_send()
    whole(qs1, 2, 8).wait_send()
    whole(qr1, 2, 8).wait_recv()
    w = base + jnp.sum(qr1[2:], axis=0)
    whole(ca, 1, 6).wait()
    sums = jnp.sum(ca[...], axis=0)
    norm0 = jnp.sum(sums[:, 1:2])
    step0 = norm0 / jnp.sum(sums[:, 0:1])
    r1 = target - step0 * w
    rr[0] = r1
    cb[0] = jnp.where(lane == 0, jnp.sum(r1 * r1), 0.0)
    for u in FAR_UNITS:
        to_user(rr, 10, u).start()
    send(rr.at[0], rr.at[1], sems.at[10], sems.at[11], partner).start()
    to_all(cb, 12)
    whole(rr, 1, 10).wait()
    whole(cb, 1, 12).wait()
    norm1 = jnp.sum(jnp.sum(cb[...], axis=0))
    beta = norm1 / norm0

    d_own = r1 + beta * target
    d_low = d_own.astype(BF16).astype(F32)

    def again(u):
        return [kt[u, 0:half], kt[u, half:]], rr[u] + beta * tu[u]

    acc = zero
    for u in (0, 1):
        acc = down(*again(u), acc)

    def second(u, carry):
        acc, curve = carry
        ks, v = again(u)
        q = across(ks, d_low)
        qs2[u] = q
        return down(ks, v, acc), curve + q * v

    carry = second(UNITS - 1, (acc, zero))
    edges = (UNITS - 2, UNITS - 24, UNITS - 44, 1)
    for hi, lo in zip(edges, edges[1:]):
        carry = lax.fori_loop(0, (hi - lo) // 2, lambda i, c, hi=hi: second(hi - 2 * i - 1, second(hi - 2 * i, c)), carry)
        for u in range(UNITS - 1 if hi == UNITS - 2 else hi, lo, -1):
            to_owner(qs2, qr2, 14, u).start()
    acc, curve = carry
    applied = acc + weight * d_own
    cc[0] = jnp.where(lane == 0, jnp.sum(d_own * applied + curve), 0.0)
    to_all(cc, 4)
    whole(qs2, 2, 14).wait_send()
    whole(qr2, 2, 14).wait_recv()
    applied = applied + jnp.sum(qr2[2:], axis=0)
    whole(cc, 1, 4).wait()
    step1 = norm1 / jnp.sum(jnp.sum(cc[...], axis=0))
    coef_out[...] = step0 * target + step1 * d_own
    res_out[...] = r1 - step1 * applied


def body(points, targets, ridge_weight):
    local, dim = points.shape
    half = local // 2
    dma = pltpu.SemaphoreType.DMA
    vec = jax.ShapeDtypeStruct((1, local), F32)
    rows = pltpu.VMEM((UNITS, 1, local), F32)
    small = pltpu.VMEM((128, 1, 128), F32)
    chunks = len(CHUNKS)
    coef, res = pl.pallas_call(
        kernel,
        out_shape=(vec, vec),
        in_specs=[
            pl.BlockSpec(memory_space=pl.ANY),
            pl.BlockSpec(memory_space=pltpu.VMEM),
            pl.BlockSpec(memory_space=pltpu.SMEM),
        ],
        out_specs=(pl.BlockSpec(memory_space=pltpu.VMEM), pl.BlockSpec(memory_space=pltpu.VMEM)),
        scratch_shapes=[
            pltpu.VMEM((dim, local), BF16),
            pltpu.VMEM((2, SLOTS, half, 2 * dim), BF16),
            pltpu.VMEM((2, SLOTS, 1, local), F32),
            rows, rows, rows, rows, rows, rows, small, small, small,
            pltpu.VMEM((4 * dim, local), BF16),
            pltpu.VMEM((4 * dim, local), BF16),
            pltpu.VMEM((UNITS, local, local), BF16),
            pltpu.VMEM((local, local), BF16),
            pltpu.VMEM((local, local), BF16),
            dma, dma((chunks,)), dma((chunks,)), dma((chunks + 1,)), dma((chunks + 1,)), dma((16,)),
            pltpu.SemaphoreType.REGULAR,
        ],
        compiler_params=pltpu.CompilerParams(
            collective_id=0, has_side_effects=True, vmem_limit_bytes=62 * 1024 * 1024),
    )(points.T, targets.reshape(1, local), ridge_weight.reshape(1, 1))
    return coef.reshape(local), res.reshape(local)


def solution(mesh):
    return jax.shard_map(
        body, mesh=mesh,
        in_specs=(P("pts", None), P("pts"), P()),
        out_specs=(P("pts"), P("pts")), check_vma=False)
```

```python
import jax
import jax.numpy as jnp
from jax import lax
from jax.experimental import pallas as pl
from jax.experimental.pallas import tpu as pltpu
from jax.sharding import PartitionSpec as P

F32 = jnp.float32
BF16 = jnp.bfloat16
TREE = (
    ((0, 0, 1), 0, 2, 1), ((0, 1, 0), 0, 1, 1), ((1, 0, 0), 0, 0, 1), ((1, 3, 0), 3, 1, -1), ((1, 1, 0), 2, 0, 1),
    ((3, 0, 1), 1, 0, -1), ((0, 1, 1), 1, 1, 1), ((0, 1, 3), 2, 2, -1), ((1, 0, 1), 3, 2, 1), ((0, 1, 2), 8, 2, -1),
    ((3, 0, 2), 6, 2, 1), ((1, 1, 1), 5, 2, 1), ((1, 2, 0), 4, 1, -1), ((1, 3, 3), 4, 2, -1), ((2, 0, 1), 6, 0, -1),
    ((2, 3, 0), 4, 0, 1), ((0, 2, 1), 7, 1, 1), ((1, 1, 3), 5, 2, -1), ((1, 3, 1), 9, 1, -1), ((1, 2, 1), 12, 1, 1),
    ((1, 2, 3), 13, 2, -1), ((3, 1, 2), 10, 0, -1), ((2, 3, 1), 15, 1, -1), ((2, 3, 3), 14, 0, 1), ((3, 3, 2), 11, 1, -1),
    ((2, 2, 1), 20, 0, 1), ((1, 2, 2), 21, 2, -1), ((2, 1, 2), 22, 0, -1), ((0, 0, 2), 1, 2, 1), ((0, 2, 0), 2, 1, 1),
    ((2, 0, 0), 3, 0, 1), ((0, 2, 2), 10, 1, 1), ((2, 0, 2), 11, 0, -1), ((2, 2, 0), 16, 1, -1), ((2, 2, 2), 26, 2, 1))
PLACES = ((0, 0, 0),) + tuple(t[0] for t in TREE)
SLOTS = len(PLACES)
SELF = 29
UNITS = 2 * SELF + SLOTS - SELF
CHUNKS = ((1, 3), (4, 6), (10, 10), (20, 6), (26, 3), (SELF, SLOTS - SELF - 1), (SLOTS - 1, 1))
LOG2E = 1.4426950408889634
ALL = tuple((z, y, x) for z in range(4) for y in range(4) for x in range(4))


def chunk_of(s):
    return [lo <= s < lo + n for lo, n in CHUNKS].index(True)


def hops(m):
    return sum(min(v, 4 - v) for v in m)


def slot_of(u):
    return (u // 2, u % 2) if u < 2 * SELF else (u - SELF, None)


FAR_UNITS = sorted(range(2, UNITS), key=lambda u: -hops(PLACES[slot_of(u)[0]]))
FAR_CHIPS = sorted(ALL, key=lambda m: -hops(m))


def kernel(pts_hbm, tgt, ridge, coef_out, res_out, bl, tl, tu, rr, qs1, qr1, qs2, qr2, ca, cb, cc,
           own_l, pacc, kt, ka, kb, sem_in, gb, gt, db, dt, sems, ack):
    me = lax.axis_index("pts")
    local = tgt.shape[1]
    dim = bl.shape[2]
    half = local // 2
    core = lax.rem(me, 2)
    chip = me // 2
    pos = (chip // 16, lax.rem(chip // 4, 4), lax.rem(chip, 4))
    axis = [[lax.rem(pos[d] + a, 4) * (32, 8, 2)[d] for a in range(4)] for d in range(3)]
    cores = (core, 1 - core)
    upper = [p // 2 for p in pos]

    def device(m, c, sign=1):
        return sum(axis[d][sign * m[d] % 4] for d in range(3)) + c

    def split(s):
        return upper[PLACES[s].index(2)]

    partner = device((0, 0, 0), cores[1])
    load = pltpu.make_async_copy(pts_hbm, bl.at[0, 0], sem_in)
    load.start()
    barrier = pltpu.get_barrier_semaphore()
    near = [partner] + [device(tuple(int(d == i) for i in range(3)), core, sign) for d in range(3) for sign in (1, -1)]
    for dev in near:
        pl.semaphore_signal(barrier, inc=1, device_id=(dev,), device_id_type=pl.DeviceIdType.MESH)

    target = tgt[...]
    t_bits = target.astype(BF16)

    load.wait()
    own_t = bl[0, 0].astype(F32)
    norm_row = jnp.sum(own_t * own_t, axis=0, keepdims=True) * (-LOG2E / dim)
    tl[0, 0] = jnp.concatenate([target, norm_row], axis=1)

    def send(src, dst, ssem, rsem, dev):
        return pltpu.make_async_remote_copy(
            src_ref=src, dst_ref=dst, send_sem=ssem, recv_sem=rsem,
            device_id=(dev,), device_id_type=pl.DeviceIdType.MESH)

    def hop(s):
        _, src, d, sign = TREE[s - 1]
        g = chunk_of(s)
        dev = device(tuple(int(d == i) for i in range(3)), core, sign)
        return (send(bl.at[0, src], bl.at[0, s], sems.at[0], gb.at[g], dev),
                send(tl.at[0, src], tl.at[0, s], sems.at[1], gt.at[g], dev))

    def across_chip(s):
        g = chunk_of(s) if s else len(CHUNKS)
        return (send(bl.at[0, s], bl.at[1, s], sems.at[2], db.at[g], partner),
                send(tl.at[0, s], tl.at[1, s], sems.at[3], dt.at[g], partner))

    def start(copies):
        for copy in copies:
            copy.start()

    def arrive(plane, g):
        lo, n = CHUNKS[g] if g < len(CHUNKS) else (0, 1)
        for buf, sem in ((bl, (gb, db)[plane]), (tl, (gt, dt)[plane])):
            ref = buf.at[plane, pl.ds(lo, n)]
            send(ref, ref, sems.at[0], sem.at[g], partner).wait_recv()

    def serve(g):
        arrive(0, g)
        lo, n = CHUNKS[g]
        for s in range(1, SLOTS):
            if lo <= TREE[s - 1][1] < lo + n:
                start(hop(s))
        for s in range(lo, lo + n):
            start(across_chip(s))
        for s in range(lo, lo + n):
            pl.semaphore_signal(ack, inc=1, device_id=(device(PLACES[s], core, -1),), device_id_type=pl.DeviceIdType.MESH)

    def whole(buf, lo, sem):
        rest = buf.at[pl.ds(lo, buf.shape[0] - lo)]
        return send(rest, rest, sems.at[sem], sems.at[sem + 1], partner)

    def to_owner(qs, qr, sem, u):
        s, plane = slot_of(u)
        c = cores[plane] if plane is not None else lax.rem(core + split(s), 2)
        return send(qs.at[u], qr.at[u], sems.at[sem], sems.at[sem + 1], device(PLACES[s], c, -1))

    def to_user(buf, sem, u):
        s, plane = slot_of(u)
        c = cores[plane] if plane is not None else lax.rem(core + 1 + split(s), 2)
        return send(buf.at[0], buf.at[u], sems.at[sem], sems.at[sem + 1], device(PLACES[s], c))

    def to_all(buf, sem):
        for m in FAR_CHIPS:
            for p in (0, 1):
                if hops(m) + p:
                    at = p * 64 + m[0] * 16 + m[1] * 4 + m[2]
                    send(buf.at[0], buf.at[at], sems.at[sem], sems.at[sem + 1], device(m, cores[p])).start()

    pl.semaphore_wait(barrier, len(near))
    for s in range(1, SLOTS):
        if TREE[s - 1][1] == 0:
            start(hop(s))
    start(across_chip(0))

    def three(x):
        hi = x.astype(BF16).astype(F32)
        mid = (x - hi).astype(BF16).astype(F32)
        return hi, mid, x - hi - mid

    def tagged(lead, then):
        rows = lax.broadcasted_iota(jnp.int32, (8, local), 0)
        out = jnp.zeros((8, local), F32)
        for i, x in enumerate(lead + then):
            out = jnp.where(rows == i, x, out)
        return jnp.concatenate([out, jnp.zeros((8, local), F32)], axis=0)

    ones = (1.0, 1.0, 1.0)
    left = jnp.concatenate([*three(own_t * (2.0 * LOG2E / dim)), tagged(ones, three(norm_row)),
                            jnp.zeros((dim - 16, local), F32)], axis=0)
    own_l[...] = left.T.astype(BF16)
    rest = jnp.zeros((dim - 16, local), BF16)

    def form(u, plane, s, keep):
        row = tl[plane, s]
        tu[u] = row[:, :local]
        pb = bl[plane, s]
        tags = tagged(three(row[:, local:]), ones).astype(BF16)
        right = jnp.concatenate([pb, pb, pb, tags, rest], axis=0)
        e = jnp.dot(own_l[...], right, preferred_element_type=F32)
        k = jnp.exp2(e).astype(BF16)
        kt[u] = k
        keep[...] = k

    def down(k, bits):
        return jnp.dot(bits, k, preferred_element_type=F32)

    def across(acc, *pairs):
        lows = [v.astype(BF16).astype(F32) for _, v in pairs]
        for r in range(0, local, 32):
            cut = pl.ds(r, 32)
            total = acc[cut]
            for (k, _), low in zip(pairs, lows):
                x = k[cut].astype(F32) * low
                total = total + ((x[:, :128] + x[:, 128:256]) + (x[:, 256:384] + x[:, 384:]))
            acc[cut] = total

    def row_of():
        return jnp.sum((pacc[0] + pacc[1]).T, axis=0, keepdims=True)

    def absorb(u, side, tw, factor=None):
        held = (ka, kb)[side]
        v = tu[u]
        q = down(held[...], t_bits)
        qs1[u] = q
        across(pacc.at[side], (held, v))
        part = q * v
        if factor is not None:
            part = part * factor
        return tw + part

    pacc[...] = jnp.zeros_like(pacc)
    form(0, 0, 0, ka)
    across(pacc.at[0], (ka, target))
    arrive(1, len(CHUNKS))
    form(1, 1, 0, kb)
    tw = jnp.zeros((1, local), F32)
    sent, ready = [], []

    def send_ready():
        for u in ready:
            to_owner(qs1, qr1, 8, u).start()
        sent.extend(ready)
        ready.clear()

    def unit_of(g, f):
        lo, n = CHUNKS[g]
        if lo >= SELF:
            plane = split(lo)
            for i in range(1, n):
                plane = jnp.where(f == i, split(lo + i), plane)
            return lo + f + SELF, plane, lo + f
        plane = jnp.where(f < n, 0, 1)
        s = lo + f - plane * n
        return 2 * s + plane, plane, s

    def run(g, last, tw, factor=None):
        lo, n = CHUNKS[g]

        def two(i, tw):
            if lo < SELF:
                @pl.when(i == n // 2)
                def _():
                    arrive(1, g)

            a, b = unit_of(g, 2 * i), unit_of(g, 2 * i + 1)
            before = jnp.where(i == 0, last, unit_of(g, 2 * i - 1)[0])
            tw = absorb(before, 1, tw, None if last > 1 else jnp.where(i == 0, 0.0, 1.0))
            form(*a, ka)
            tw = absorb(a[0], 0, tw)
            form(*b, kb)
            return tw

        tw = lax.fori_loop(0, n if lo < SELF else n // 2, two, tw)
        units = [s + SELF for s in range(lo, lo + n)] if lo >= SELF else (
            [2 * s for s in range(lo, lo + n)] + [2 * s + 1 for s in range(lo, lo + n)])
        if last > 1:
            ready.append(last)
        ready.extend(units[:-1])
        return units[-1], tw

    last = 1
    for g in range(5):
        serve(g)
        send_ready()
        if g < 4:
            last, tw = run(g, last, tw)
    serve(5)
    arrive(1, 5)
    last, tw = run(5, last, tw)
    serve(6)
    send_ready()
    last, tw = run(4, last, tw)
    arrive(1, 6)
    tw = absorb(last, 1, tw)
    form(UNITS - 1, split(SLOTS - 1), SLOTS - 1, ka)
    tw = absorb(UNITS - 1, 0, tw)
    ready.extend((last, UNITS - 1))

    ready.reverse()
    send_ready()
    weight = ridge[0, 0]
    base = row_of() + weight * target
    lane = lax.broadcasted_iota(jnp.int32, (1, 128), 1)
    ca[0] = jnp.where(lane == 0, jnp.sum(tw + target * base), jnp.where(lane == 1, jnp.sum(target * target), 0.0))
    pl.semaphore_wait(ack, SLOTS - 1)
    to_all(ca, 6)
    moved = bl.at[0, pl.ds(1, SLOTS - 1)], tl.at[0, pl.ds(1, SLOTS - 1)], bl.at[0], tl.at[0]
    for i, ref in enumerate(moved):
        send(ref, ref, sems.at[i], sem_in, partner).wait_send()
    whole(qs1, 2, 8).wait_send()
    whole(qr1, 2, 8).wait_recv()
    w = base + jnp.sum(qr1[2:], axis=0)
    whole(ca, 1, 6).wait()
    sums = jnp.sum(ca[...], axis=0)
    norm0 = jnp.sum(sums[:, 1:2])
    step0 = norm0 / jnp.sum(sums[:, 0:1])
    r1 = target - step0 * w
    rr[0] = r1
    cb[0] = jnp.where(lane == 0, jnp.sum(r1 * r1), 0.0)
    for u in FAR_UNITS:
        to_user(rr, 10, u).start()
    send(rr.at[0], rr.at[1], sems.at[10], sems.at[11], partner).start()
    to_all(cb, 12)
    whole(rr, 1, 10).wait()
    whole(cb, 1, 12).wait()
    norm1 = jnp.sum(jnp.sum(cb[...], axis=0))
    beta = norm1 / norm0

    d_own = r1 + beta * target
    d_bits = d_own.astype(BF16)
    pacc[...] = jnp.zeros_like(pacc)

    def again(u):
        return kt.at[u], rr[u] + beta * tu[u]

    across(pacc.at[0], again(0), again(1))

    def second(curve, *units):
        pairs = [again(u) for u in units]
        for u, (k, v) in zip(units, pairs):
            q = down(k[...], d_bits)
            qs2[u] = q
            curve = curve + q * v
        across(pacc.at[0], *pairs)
        return curve

    curve = second(jnp.zeros((1, local), F32), UNITS - 1)
    edges = (UNITS - 2, UNITS - 24, UNITS - 44, 1)
    for hi, lo in zip(edges, edges[1:]):
        curve = lax.fori_loop(0, (hi - lo) // 2, lambda i, c, hi=hi: second(c, hi - 2 * i, hi - 2 * i - 1), curve)
        for u in range(UNITS - 1 if hi == UNITS - 2 else hi, lo, -1):
            to_owner(qs2, qr2, 14, u).start()
    applied = row_of() + weight * d_own
    cc[0] = jnp.where(lane == 0, jnp.sum(d_own * applied + curve), 0.0)
    to_all(cc, 4)
    whole(qs2, 2, 14).wait_send()
    whole(qr2, 2, 14).wait_recv()
    applied = applied + jnp.sum(qr2[2:], axis=0)
    whole(cc, 1, 4).wait()
    step1 = norm1 / jnp.sum(jnp.sum(cc[...], axis=0))
    coef_out[...] = step0 * target + step1 * d_own
    res_out[...] = r1 - step1 * applied


def body(points, targets, ridge_weight):
    local, dim = points.shape
    dma = pltpu.SemaphoreType.DMA
    vec = jax.ShapeDtypeStruct((1, local), F32)
    rows = pltpu.VMEM((UNITS, 1, local), F32)
    small = pltpu.VMEM((128, 1, 128), F32)
    chunks = len(CHUNKS)
    coef, res = pl.pallas_call(
        kernel,
        out_shape=(vec, vec),
        in_specs=[
            pl.BlockSpec(memory_space=pl.ANY),
            pl.BlockSpec(memory_space=pltpu.VMEM),
            pl.BlockSpec(memory_space=pltpu.SMEM),
        ],
        out_specs=(pl.BlockSpec(memory_space=pltpu.VMEM), pl.BlockSpec(memory_space=pltpu.VMEM)),
        scratch_shapes=[
            pltpu.VMEM((2, SLOTS, dim, local), BF16),
            pltpu.VMEM((2, SLOTS, 1, 2 * local), F32),
            rows, rows, rows, rows, rows, rows, small, small, small,
            pltpu.VMEM((local, 4 * dim), BF16),
            pltpu.VMEM((2, local, 128), F32),
            pltpu.VMEM((UNITS, local, local), BF16),
            pltpu.VMEM((local, local), BF16),
            pltpu.VMEM((local, local), BF16),
            dma, dma((chunks,)), dma((chunks,)), dma((chunks + 1,)), dma((chunks + 1,)), dma((16,)),
            pltpu.SemaphoreType.REGULAR,
        ],
        compiler_params=pltpu.CompilerParams(
            collective_id=0, has_side_effects=True, vmem_limit_bytes=62 * 1024 * 1024),
    )(points.T, targets.reshape(1, local), ridge_weight.reshape(1, 1))
    return coef.reshape(local), res.reshape(local)


def solution(mesh):
    return jax.shard_map(
        body, mesh=mesh,
        in_specs=(P("pts", None), P("pts"), P()),
        out_specs=(P("pts"), P("pts")), check_vma=False)
```

```python
import jax
import jax.numpy as jnp
from jax import lax
from jax.experimental import pallas as pl
from jax.experimental.pallas import tpu as pltpu
from jax.sharding import PartitionSpec as P

F32 = jnp.float32
BF16 = jnp.bfloat16
TREE = (
    ((0, 0, 1), 0, 2, 1), ((0, 1, 0), 0, 1, 1), ((1, 0, 0), 0, 0, 1), ((1, 3, 0), 3, 1, -1), ((1, 1, 0), 2, 0, 1),
    ((3, 0, 1), 1, 0, -1), ((0, 1, 1), 1, 1, 1), ((0, 1, 3), 2, 2, -1), ((1, 0, 1), 3, 2, 1), ((0, 1, 2), 8, 2, -1),
    ((3, 0, 2), 6, 2, 1), ((1, 1, 1), 5, 2, 1), ((1, 2, 0), 4, 1, -1), ((1, 3, 3), 4, 2, -1), ((2, 0, 1), 6, 0, -1),
    ((2, 3, 0), 4, 0, 1), ((0, 2, 1), 7, 1, 1), ((1, 1, 3), 5, 2, -1), ((1, 3, 1), 9, 1, -1), ((1, 2, 1), 12, 1, 1),
    ((1, 2, 3), 13, 2, -1), ((3, 1, 2), 10, 0, -1), ((2, 3, 1), 15, 1, -1), ((2, 3, 3), 14, 0, 1), ((3, 3, 2), 11, 1, -1),
    ((2, 2, 1), 20, 0, 1), ((1, 2, 2), 21, 2, -1), ((2, 1, 2), 22, 0, -1), ((0, 0, 2), 1, 2, 1), ((0, 2, 0), 2, 1, 1),
    ((2, 0, 0), 3, 0, 1), ((0, 2, 2), 10, 1, 1), ((2, 0, 2), 11, 0, -1), ((2, 2, 0), 16, 1, -1), ((2, 2, 2), 26, 2, 1))
PLACES = ((0, 0, 0),) + tuple(t[0] for t in TREE)
SLOTS = len(PLACES)
SELF = 29
UNITS = 2 * SELF + SLOTS - SELF
CHUNKS = ((1, 3), (4, 6), (10, 4), (14, 6), (20, 6), (26, 3), (SELF, SLOTS - SELF - 1), (SLOTS - 1, 1))
LOG2E = 1.4426950408889634
PLAN = ((0, (0,), 6), (1, (1,), 6), (2, (2,), 4), (3, (3, 4), 6), (4, (5,), 6), (6, (6,), 6), (5, (), 6))
ALL = tuple((z, y, x) for z in range(4) for y in range(4) for x in range(4))


def chunk_of(s):
    return [lo <= s < lo + n for lo, n in CHUNKS].index(True)


def hops(m):
    return sum(min(v, 4 - v) for v in m)


def slot_of(u):
    return (u // 2, u % 2) if u < 2 * SELF else (u - SELF, None)


FAR_UNITS = sorted(range(2, UNITS), key=lambda u: -hops(PLACES[slot_of(u)[0]]))
FAR_CHIPS = sorted(ALL, key=lambda m: -hops(m))


def kernel(pts_hbm, tgt, ridge, coef_out, res_out, bl, tl, tu, rr, qs1, qr1, qs2, qr2, ca, cb, cc,
           own_l, pacc, kt, ka, kb, sem_in, gb, gt, db, dt, sems, ack):
    me = lax.axis_index("pts")
    local = tgt.shape[1]
    dim = bl.shape[2]
    half = local // 2
    core = lax.rem(me, 2)
    chip = me // 2
    pos = (chip // 16, lax.rem(chip // 4, 4), lax.rem(chip, 4))
    axis = [[lax.rem(pos[d] + a, 4) * (32, 8, 2)[d] for a in range(4)] for d in range(3)]
    cores = (core, 1 - core)
    upper = [p // 2 for p in pos]

    def device(m, c, sign=1):
        return sum(axis[d][sign * m[d] % 4] for d in range(3)) + c

    def split(s):
        return upper[PLACES[s].index(2)]

    partner = device((0, 0, 0), cores[1])
    load = pltpu.make_async_copy(pts_hbm, bl.at[0, 0], sem_in)
    load.start()
    barrier = pltpu.get_barrier_semaphore()
    near = [partner] + [device(tuple(int(d == i) for i in range(3)), core, sign) for d in range(3) for sign in (1, -1)]
    for dev in near:
        pl.semaphore_signal(barrier, inc=1, device_id=(dev,), device_id_type=pl.DeviceIdType.MESH)

    target = tgt[...]
    t_bits = target.astype(BF16)

    load.wait()
    own_t = bl[0, 0].astype(F32)
    norm_row = jnp.sum(own_t * own_t, axis=0, keepdims=True) * (-LOG2E / dim)
    tl[0, 0] = jnp.concatenate([target, norm_row], axis=1)

    def send(src, dst, ssem, rsem, dev):
        return pltpu.make_async_remote_copy(
            src_ref=src, dst_ref=dst, send_sem=ssem, recv_sem=rsem,
            device_id=(dev,), device_id_type=pl.DeviceIdType.MESH)

    def hop(s):
        _, src, d, sign = TREE[s - 1]
        g = chunk_of(s)
        dev = device(tuple(int(d == i) for i in range(3)), core, sign)
        return (send(bl.at[0, src], bl.at[0, s], sems.at[0], gb.at[g], dev),
                send(tl.at[0, src], tl.at[0, s], sems.at[1], gt.at[g], dev))

    def across_chip(s):
        g = chunk_of(s) if s else len(CHUNKS)
        return (send(bl.at[0, s], bl.at[1, s], sems.at[2], db.at[g], partner),
                send(tl.at[0, s], tl.at[1, s], sems.at[3], dt.at[g], partner))

    def start(copies):
        for copy in copies:
            copy.start()

    def arrive(plane, g):
        lo, n = CHUNKS[g] if g < len(CHUNKS) else (0, 1)
        for buf, sem in ((bl, (gb, db)[plane]), (tl, (gt, dt)[plane])):
            ref = buf.at[plane, pl.ds(lo, n)]
            send(ref, ref, sems.at[0], sem.at[g], partner).wait_recv()

    def serve(g):
        arrive(0, g)
        lo, n = CHUNKS[g]
        for s in range(1, SLOTS):
            if lo <= TREE[s - 1][1] < lo + n:
                start(hop(s))
        for s in range(lo, lo + n):
            start(across_chip(s))
        for s in range(lo, lo + n):
            pl.semaphore_signal(ack, inc=1, device_id=(device(PLACES[s], core, -1),), device_id_type=pl.DeviceIdType.MESH)

    def whole(buf, lo, sem):
        rest = buf.at[pl.ds(lo, buf.shape[0] - lo)]
        return send(rest, rest, sems.at[sem], sems.at[sem + 1], partner)

    def to_owner(qs, qr, sem, u):
        s, plane = slot_of(u)
        c = cores[plane] if plane is not None else lax.rem(core + split(s), 2)
        return send(qs.at[u], qr.at[u], sems.at[sem], sems.at[sem + 1], device(PLACES[s], c, -1))

    def to_user(buf, sem, u):
        s, plane = slot_of(u)
        c = cores[plane] if plane is not None else lax.rem(core + 1 + split(s), 2)
        return send(buf.at[0], buf.at[u], sems.at[sem], sems.at[sem + 1], device(PLACES[s], c))

    def to_all(buf, sem):
        for m in FAR_CHIPS:
            for p in (0, 1):
                if hops(m) + p:
                    at = p * 64 + m[0] * 16 + m[1] * 4 + m[2]
                    send(buf.at[0], buf.at[at], sems.at[sem], sems.at[sem + 1], device(m, cores[p])).start()

    pl.semaphore_wait(barrier, len(near))
    for s in range(1, SLOTS):
        if TREE[s - 1][1] == 0:
            start(hop(s))
    start(across_chip(0))

    def three(x):
        hi = x.astype(BF16).astype(F32)
        mid = (x - hi).astype(BF16).astype(F32)
        return hi, mid, x - hi - mid

    def tagged(lead, then):
        rows = lax.broadcasted_iota(jnp.int32, (8, local), 0)
        out = jnp.zeros((8, local), F32)
        for i, x in enumerate(lead + then):
            out = jnp.where(rows == i, x, out)
        return jnp.concatenate([out, jnp.zeros((8, local), F32)], axis=0)

    ones = (1.0, 1.0, 1.0)
    left = jnp.concatenate([*three(own_t * (2.0 * LOG2E / dim)), tagged(ones, three(norm_row)),
                            jnp.zeros((dim - 16, local), F32)], axis=0)
    own_l[...] = left.T.astype(BF16)
    rest = jnp.zeros((dim - 16, local), BF16)

    def power(u, plane, s):
        row = tl[plane, s]
        tu[u] = row[:, :local]
        pb = bl[plane, s]
        tags = tagged(three(row[:, local:]), ones).astype(BF16)
        right = jnp.concatenate([pb, pb, pb, tags, rest], axis=0)
        return jnp.dot(own_l[...], right, preferred_element_type=F32)

    def keep(u, e, side):
        for r in range(0, local, 32):
            k = jnp.exp2(e[r:r + 32]).astype(BF16)
            kt[u, r:r + 32] = k
            (ka, kb)[side][r:r + 32] = k

    def down(k, bits):
        return jnp.dot(bits, k, preferred_element_type=F32)

    def across(acc, *pairs):
        lows = [v.astype(BF16).astype(F32) for _, v in pairs]
        for r in range(0, local, 16):
            cut = pl.ds(r, 16)
            total = acc[cut]
            for (k, _), low in zip(pairs, lows):
                x = k[cut].astype(F32) * low
                total = total + ((x[:, :128] + x[:, 128:256]) + (x[:, 256:384] + x[:, 384:]))
            acc[cut] = total

    def row_of():
        return jnp.sum((pacc[0] + pacc[1]).T, axis=0, keepdims=True)

    def absorb(u, side, tw, factor=None):
        held = (ka, kb)[side]
        v = tu[u]
        q = down(held[...], t_bits)
        qs1[u] = q
        across(pacc.at[side], (held, v))
        part = q * v
        if factor is not None:
            part = part * factor
        return tw + part

    pacc[...] = jnp.zeros_like(pacc)
    keep(0, power(0, 0, 0), 0)
    across(pacc.at[0], (ka, target))
    arrive(1, len(CHUNKS))
    keep(1, power(1, 1, 0), 1)
    tw = jnp.zeros((1, local), F32)
    sent, ready = [], []

    def send_ready():
        for u in ready:
            to_owner(qs1, qr1, 8, u).start()
        sent.extend(ready)
        ready.clear()

    def unit_of(g, f):
        lo, n = CHUNKS[g]
        if lo >= SELF:
            plane = split(lo)
            for i in range(1, n):
                plane = jnp.where(f == i, split(lo + i), plane)
            return lo + f + SELF, plane, lo + f
        plane = jnp.where(f < n, 0, 1)
        s = lo + f - plane * n
        return 2 * s + plane, plane, s

    def run(g, last, tw, width):
        lo, n = CHUNKS[g]
        count = n if lo >= SELF else 2 * n

        def some(i, tw):
            if lo < SELF:
                @pl.when(i == n // width)
                def _():
                    arrive(1, g)

            units = [unit_of(g, width * i + j) for j in range(width)]
            before = jnp.where(i == 0, last, unit_of(g, width * i - 1)[0])
            factor = None if last > 1 else jnp.where(i == 0, 0.0, 1.0)
            e = power(*units[0])
            for j in range(width):
                ahead = power(*units[j + 1]) if j + 1 < width else None
                tw = absorb(units[j - 1][0] if j else before, 1 - j % 2, tw, None if j else factor)
                keep(units[j][0], e, j % 2)
                e = ahead
            return tw

        tw = lax.fori_loop(0, count // width, some, tw)
        units = [s + SELF for s in range(lo, lo + n)] if lo >= SELF else (
            [2 * s for s in range(lo, lo + n)] + [2 * s + 1 for s in range(lo, lo + n)])
        if last > 1:
            ready.append(last)
        ready.extend(units[:-1])
        return units[-1], tw

    last = 1
    for g, then, width in PLAN:
        for h in then:
            serve(h)
            if h >= 6:
                arrive(1, h)
        send_ready()
        last, tw = run(g, last, tw, width)
    serve(7)
    arrive(1, 7)
    e = power(UNITS - 1, split(SLOTS - 1), SLOTS - 1)
    tw = absorb(last, 1, tw)
    keep(UNITS - 1, e, 0)
    tw = absorb(UNITS - 1, 0, tw)
    ready.extend((last, UNITS - 1))

    ready.reverse()
    send_ready()
    weight = ridge[0, 0]
    base = row_of() + weight * target
    lane = lax.broadcasted_iota(jnp.int32, (1, 128), 1)
    ca[0] = jnp.where(lane == 0, jnp.sum(tw + target * base), jnp.where(lane == 1, jnp.sum(target * target), 0.0))
    pl.semaphore_wait(ack, SLOTS - 1)
    to_all(ca, 6)
    moved = bl.at[0, pl.ds(1, SLOTS - 1)], tl.at[0, pl.ds(1, SLOTS - 1)], bl.at[0], tl.at[0]
    for i, ref in enumerate(moved):
        send(ref, ref, sems.at[i], sem_in, partner).wait_send()
    whole(qs1, 2, 8).wait_send()
    whole(qr1, 2, 8).wait_recv()
    w = base + jnp.sum(qr1[2:], axis=0)
    whole(ca, 1, 6).wait()
    sums = jnp.sum(ca[...], axis=0)
    norm0 = jnp.sum(sums[:, 1:2])
    step0 = norm0 / jnp.sum(sums[:, 0:1])
    r1 = target - step0 * w
    rr[0] = r1
    cb[0] = jnp.where(lane == 0, jnp.sum(r1 * r1), 0.0)
    for u in FAR_UNITS:
        to_user(rr, 10, u).start()
    send(rr.at[0], rr.at[1], sems.at[10], sems.at[11], partner).start()
    to_all(cb, 12)
    whole(rr, 1, 10).wait()
    whole(cb, 1, 12).wait()
    norm1 = jnp.sum(jnp.sum(cb[...], axis=0))
    beta = norm1 / norm0

    d_own = r1 + beta * target
    d_bits = d_own.astype(BF16)
    pacc[...] = jnp.zeros_like(pacc)

    def again(u):
        return kt.at[u], rr[u] + beta * tu[u]

    across(pacc.at[0], again(0), again(1))

    def second(curve, *units):
        pairs = [again(u) for u in units]
        for u, (k, v) in zip(units, pairs):
            q = down(k[...], d_bits)
            qs2[u] = q
            curve = curve + q * v
        across(pacc.at[0], *pairs)
        return curve

    curve = second(jnp.zeros((1, local), F32), UNITS - 1)
    edges = (UNITS - 2, UNITS - 24, UNITS - 44, 1)
    for hi, lo in zip(edges, edges[1:]):
        curve = lax.fori_loop(0, (hi - lo) // 2, lambda i, c, hi=hi: second(c, hi - 2 * i, hi - 2 * i - 1), curve)
        for u in range(UNITS - 1 if hi == UNITS - 2 else hi, lo, -1):
            to_owner(qs2, qr2, 14, u).start()
    applied = row_of() + weight * d_own
    cc[0] = jnp.where(lane == 0, jnp.sum(d_own * applied + curve), 0.0)
    to_all(cc, 4)
    whole(qs2, 2, 14).wait_send()
    whole(qr2, 2, 14).wait_recv()
    applied = applied + jnp.sum(qr2[2:], axis=0)
    whole(cc, 1, 4).wait()
    step1 = norm1 / jnp.sum(jnp.sum(cc[...], axis=0))
    coef_out[...] = step0 * target + step1 * d_own
    res_out[...] = r1 - step1 * applied


def body(points, targets, ridge_weight):
    local, dim = points.shape
    dma = pltpu.SemaphoreType.DMA
    vec = jax.ShapeDtypeStruct((1, local), F32)
    rows = pltpu.VMEM((UNITS, 1, local), F32)
    small = pltpu.VMEM((128, 1, 128), F32)
    chunks = len(CHUNKS)
    coef, res = pl.pallas_call(
        kernel,
        out_shape=(vec, vec),
        in_specs=[
            pl.BlockSpec(memory_space=pl.ANY),
            pl.BlockSpec(memory_space=pltpu.VMEM),
            pl.BlockSpec(memory_space=pltpu.SMEM),
        ],
        out_specs=(pl.BlockSpec(memory_space=pltpu.VMEM), pl.BlockSpec(memory_space=pltpu.VMEM)),
        scratch_shapes=[
            pltpu.VMEM((2, SLOTS, dim, local), BF16),
            pltpu.VMEM((2, SLOTS, 1, 2 * local), F32),
            rows, rows, rows, rows, rows, rows, small, small, small,
            pltpu.VMEM((local, 4 * dim), BF16),
            pltpu.VMEM((2, local, 128), F32),
            pltpu.VMEM((UNITS, local, local), BF16),
            pltpu.VMEM((local, local), BF16),
            pltpu.VMEM((local, local), BF16),
            dma, dma((chunks,)), dma((chunks,)), dma((chunks + 1,)), dma((chunks + 1,)), dma((16,)),
            pltpu.SemaphoreType.REGULAR,
        ],
        compiler_params=pltpu.CompilerParams(
            collective_id=0, has_side_effects=True, vmem_limit_bytes=62 * 1024 * 1024),
    )(points.T, targets.reshape(1, local), ridge_weight.reshape(1, 1))
    return coef.reshape(local), res.reshape(local)


def solution(mesh):
    return jax.shard_map(
        body, mesh=mesh,
        in_specs=(P("pts", None), P("pts"), P()),
        out_specs=(P("pts"), P("pts")), check_vma=False)
```

```python
import jax
import jax.numpy as jnp
from jax import lax
from jax.experimental import pallas as pl
from jax.experimental.pallas import tpu as pltpu
from jax.sharding import PartitionSpec as P

F32 = jnp.float32
BF16 = jnp.bfloat16
TREE = (
    ((0, 0, 1), 0, 2, 1), ((0, 1, 0), 0, 1, 1), ((1, 0, 0), 0, 0, 1), ((1, 3, 0), 3, 1, -1), ((1, 1, 0), 2, 0, 1),
    ((3, 0, 1), 1, 0, -1), ((0, 1, 1), 1, 1, 1), ((0, 1, 3), 2, 2, -1), ((1, 0, 1), 3, 2, 1), ((0, 1, 2), 8, 2, -1),
    ((3, 0, 2), 6, 2, 1), ((1, 1, 1), 5, 2, 1), ((1, 2, 0), 4, 1, -1), ((1, 3, 3), 4, 2, -1), ((2, 0, 1), 6, 0, -1),
    ((2, 3, 0), 4, 0, 1), ((0, 2, 1), 7, 1, 1), ((1, 1, 3), 5, 2, -1), ((1, 3, 1), 9, 1, -1), ((1, 2, 1), 12, 1, 1),
    ((1, 2, 3), 13, 2, -1), ((3, 1, 2), 10, 0, -1), ((2, 3, 1), 15, 1, -1), ((2, 3, 3), 14, 0, 1), ((3, 3, 2), 11, 1, -1),
    ((2, 2, 1), 20, 0, 1), ((1, 2, 2), 21, 2, -1), ((2, 1, 2), 22, 0, -1), ((0, 0, 2), 1, 2, 1), ((0, 2, 0), 2, 1, 1),
    ((2, 0, 0), 3, 0, 1), ((0, 2, 2), 10, 1, 1), ((2, 0, 2), 11, 0, -1), ((2, 2, 0), 16, 1, -1), ((2, 2, 2), 26, 2, 1))
PLACES = ((0, 0, 0),) + tuple(t[0] for t in TREE)
SLOTS = len(PLACES)
SELF = 29
UNITS = 2 * SELF + SLOTS - SELF
CHUNKS = ((1, 3), (4, 6), (10, 10), (20, 6), (26, 3), (29, 3), (32, 3), (35, 1))
LOG2E = 1.4426950408889634


def plane_of(plane, lo, hi):
    return tuple((s, plane) for s in range(lo, hi))


PLAN = (
    ((0,), (), plane_of(0, 1, 4)),
    ((), (0,), plane_of(1, 1, 4)),
    ((1,), (), plane_of(0, 4, 10)),
    ((5,), (1,), plane_of(1, 4, 10)),
    ((2,), (5,), plane_of(0, 10, 16)),
    ((), (), plane_of(0, 16, 20) + plane_of(None, 29, 31)),
    ((3,), (2,), plane_of(1, 10, 16)),
    ((6,), (), plane_of(1, 16, 20) + plane_of(None, 31, 32)),
    ((4,), (), plane_of(0, 20, 26)),
    ((), (3, 6), plane_of(1, 20, 26)),
    ((7,), (4,), plane_of(0, 26, 29) + plane_of(1, 26, 29)),
    ((), (7,), plane_of(None, 32, 36)))
ALL = tuple((z, y, x) for z in range(4) for y in range(4) for x in range(4))


def chunk_of(s):
    return [lo <= s < lo + n for lo, n in CHUNKS].index(True)


def hops(m):
    return sum(min(v, 4 - v) for v in m)


def slot_of(u):
    return (u // 2, u % 2) if u < 2 * SELF else (u - SELF, None)


FAR = 40
FAR_UNITS = sorted(range(2, UNITS), key=lambda u: -hops(PLACES[slot_of(u)[0]]))
FAR_CHIPS = sorted(ALL, key=lambda m: -hops(m))


def kernel(pts_hbm, tgt, ridge, coef_out, res_out, bl, tl, tu, rr, qs1, qr1, qs2, qr2, ca, cb, cc,
           own_l, pacc, kt, ka, kb, sem_in, gb, gt, db, dt, sems, ack):
    me = lax.axis_index("pts")
    local = tgt.shape[1]
    dim = bl.shape[2]
    half = local // 2
    core = lax.rem(me, 2)
    chip = me // 2
    pos = (chip // 16, lax.rem(chip // 4, 4), lax.rem(chip, 4))
    axis = [[lax.rem(pos[d] + a, 4) * (32, 8, 2)[d] for a in range(4)] for d in range(3)]
    cores = (core, 1 - core)
    upper = [p // 2 for p in pos]

    def device(m, c, sign=1):
        return sum(axis[d][sign * m[d] % 4] for d in range(3)) + c

    def split(s):
        return upper[PLACES[s].index(2)]

    partner = device((0, 0, 0), cores[1])
    load = pltpu.make_async_copy(pts_hbm, bl.at[0, 0], sem_in)
    load.start()
    barrier = pltpu.get_barrier_semaphore()
    near = [partner] + [device(tuple(int(d == i) for i in range(3)), core, sign) for d in range(3) for sign in (1, -1)]
    for dev in near:
        pl.semaphore_signal(barrier, inc=1, device_id=(dev,), device_id_type=pl.DeviceIdType.MESH)

    target = tgt[...]
    t_bits = target.astype(BF16)

    load.wait()
    own_t = bl[0, 0].astype(F32)
    norm_row = jnp.sum(own_t * own_t, axis=0, keepdims=True) * (-LOG2E / dim)
    tl[0, 0] = jnp.concatenate([target, norm_row], axis=1)

    def send(src, dst, ssem, rsem, dev):
        return pltpu.make_async_remote_copy(
            src_ref=src, dst_ref=dst, send_sem=ssem, recv_sem=rsem,
            device_id=(dev,), device_id_type=pl.DeviceIdType.MESH)

    def hop(s):
        _, src, d, sign = TREE[s - 1]
        g = chunk_of(s)
        dev = device(tuple(int(d == i) for i in range(3)), core, sign)
        return (send(bl.at[0, src], bl.at[0, s], sems.at[0], gb.at[g], dev),
                send(tl.at[0, src], tl.at[0, s], sems.at[1], gt.at[g], dev))

    def across_chip(s):
        g = chunk_of(s) if s else len(CHUNKS)
        return (send(bl.at[0, s], bl.at[1, s], sems.at[2], db.at[g], partner),
                send(tl.at[0, s], tl.at[1, s], sems.at[3], dt.at[g], partner))

    def start(copies):
        for copy in copies:
            copy.start()

    def arrive(plane, g):
        lo, n = CHUNKS[g] if g < len(CHUNKS) else (0, 1)
        for buf, sem in ((bl, (gb, db)[plane]), (tl, (gt, dt)[plane])):
            ref = buf.at[plane, pl.ds(lo, n)]
            send(ref, ref, sems.at[0], sem.at[g], partner).wait_recv()

    def serve(g):
        arrive(0, g)
        lo, n = CHUNKS[g]
        for s in range(1, SLOTS):
            if lo <= TREE[s - 1][1] < lo + n:
                start(hop(s))
        for s in range(lo, lo + n):
            start(across_chip(s))
        for s in range(lo, lo + n):
            pl.semaphore_signal(ack, inc=1, device_id=(device(PLACES[s], core, -1),), device_id_type=pl.DeviceIdType.MESH)

    def whole(buf, lo, sem):
        rest = buf.at[pl.ds(lo, buf.shape[0] - lo)]
        return send(rest, rest, sems.at[sem], sems.at[sem + 1], partner)

    def to_owner(qs, qr, sem, u):
        s, plane = slot_of(u)
        c = cores[plane] if plane is not None else lax.rem(core + split(s), 2)
        return send(qs.at[u], qr.at[u], sems.at[sem], sems.at[sem + 1], device(PLACES[s], c, -1))

    def to_user(buf, sem, u):
        s, plane = slot_of(u)
        c = cores[plane] if plane is not None else lax.rem(core + 1 + split(s), 2)
        return send(buf.at[0], buf.at[u], sems.at[sem], sems.at[sem + 1], device(PLACES[s], c))

    def to_all(buf, sem):
        for m in FAR_CHIPS:
            for p in (0, 1):
                if hops(m) + p:
                    at = p * 64 + m[0] * 16 + m[1] * 4 + m[2]
                    send(buf.at[0], buf.at[at], sems.at[sem], sems.at[sem + 1], device(m, cores[p])).start()

    pl.semaphore_wait(barrier, len(near))
    for s in range(1, SLOTS):
        if TREE[s - 1][1] == 0:
            start(hop(s))
    start(across_chip(0))

    def three(x):
        hi = x.astype(BF16).astype(F32)
        mid = (x - hi).astype(BF16).astype(F32)
        return hi, mid, x - hi - mid

    def tagged(lead, then):
        rows = lax.broadcasted_iota(jnp.int32, (8, local), 0)
        out = jnp.zeros((8, local), F32)
        for i, x in enumerate(lead + then):
            out = jnp.where(rows == i, x, out)
        return jnp.concatenate([out, jnp.zeros((8, local), F32)], axis=0)

    ones = (1.0, 1.0, 1.0)
    left = jnp.concatenate([*three(own_t * (2.0 * LOG2E / dim)), tagged(ones, three(norm_row)),
                            jnp.zeros((dim - 16, local), F32)], axis=0)
    own_l[...] = left.T.astype(BF16)
    rest = jnp.zeros((dim - 16, local), BF16)

    def power(u, plane, s):
        row = tl[plane, s]
        tu[u] = row[:, :local]
        pb = bl[plane, s]
        tags = tagged(three(row[:, local:]), ones).astype(BF16)
        right = jnp.concatenate([pb, pb, pb, tags, rest], axis=0)
        return jnp.dot(own_l[...], right, preferred_element_type=F32)

    def keep(u, e, side):
        for r in range(0, local, 32):
            k = jnp.exp2(e[r:r + 32]).astype(BF16)
            kt[u, r:r + 32] = k
            (ka, kb)[side][r:r + 32] = k

    def down(k, bits):
        return jnp.dot(bits, k, preferred_element_type=F32)

    def across(acc, *pairs):
        lows = [v.astype(BF16).astype(F32) for _, v in pairs]
        for r in range(0, local, 16):
            cut = pl.ds(r, 16)
            total = acc[cut]
            for (k, _), low in zip(pairs, lows):
                for c in range(0, local, 128):
                    total = total + k[cut, c:c + 128].astype(F32) * low[:, c:c + 128]
            acc[cut] = total

    def row_of():
        return jnp.sum((pacc[0] + pacc[1]).T, axis=0, keepdims=True)

    def absorb(u, side, tw):
        held = (ka, kb)[side]
        v = tu[u]
        q = None
        if u > 1:
            q = down(held[...], t_bits)
            qs1[u] = q
        across(pacc.at[side], (held, v))
        return tw if q is None else tw + q * v

    pacc[...] = jnp.zeros_like(pacc)
    keep(0, power(0, 0, 0), 0)
    across(pacc.at[0], (ka, target))
    arrive(1, len(CHUNKS))
    keep(1, power(1, 1, 0), 1)
    tw = jnp.zeros((1, local), F32)
    sent, ready = [], []

    def send_ready():
        for u in ready:
            to_owner(qs1, qr1, 8, u).start()
        sent.extend(ready)
        ready.clear()

    prev, count = 1, 1
    for served, crossed, units in PLAN:
        for g in served:
            serve(g)
        for g in crossed:
            arrive(1, g)
        send_ready()
        units = [(s + SELF, split(s), s) if plane is None else (2 * s + plane, plane, s) for s, plane in units]
        e = power(*units[0])
        for j, (u, _, _) in enumerate(units):
            ahead = power(*units[j + 1]) if j + 1 < len(units) else None
            tw = absorb(prev, count % 2, tw)
            if prev > 1:
                ready.append(prev)
            count += 1
            keep(u, e, count % 2)
            prev, e = u, ahead

    tw = absorb(prev, count % 2, tw)
    ready.append(prev)

    ready.reverse()
    send_ready()
    weight = ridge[0, 0]
    base = row_of() + weight * target
    lane = lax.broadcasted_iota(jnp.int32, (1, 128), 1)
    ca[0] = jnp.where(lane == 0, jnp.sum(tw + target * base), jnp.where(lane == 1, jnp.sum(target * target), 0.0))
    pl.semaphore_wait(ack, SLOTS - 1)
    to_all(ca, 6)
    moved = bl.at[0, pl.ds(1, SLOTS - 1)], tl.at[0, pl.ds(1, SLOTS - 1)], bl.at[0], tl.at[0]
    for i, ref in enumerate(moved):
        send(ref, ref, sems.at[i], sem_in, partner).wait_send()
    whole(qs1, 2, 8).wait_send()
    whole(qr1, 2, 8).wait_recv()
    w = base + jnp.sum(qr1[2:], axis=0)
    whole(ca, 1, 6).wait()
    sums = jnp.sum(ca[...], axis=0)
    norm0 = jnp.sum(sums[:, 1:2])
    step0 = norm0 / jnp.sum(sums[:, 0:1])
    r1 = target - step0 * w
    rr[0] = r1
    cb[0] = jnp.where(lane == 0, jnp.sum(r1 * r1), 0.0)
    to_all(cb, 12)
    for u in FAR_UNITS:
        to_user(rr, 16 if u >= FAR else 10, u).start()
    send(rr.at[0], rr.at[1], sems.at[10], sems.at[11], partner).start()
    whole(cb, 1, 12).wait()
    norm1 = jnp.sum(jnp.sum(cb[...], axis=0))
    beta = norm1 / norm0
    whole(rr.at[pl.ds(0, FAR)], 1, 10).wait()

    d_own = r1 + beta * target
    d_bits = d_own.astype(BF16)
    pacc[...] = jnp.zeros_like(pacc)

    def again(u):
        return kt.at[u], rr[u] + beta * tu[u]

    across(pacc.at[0], again(0), again(1))

    def second(curve, *units):
        pairs = [again(u) for u in units]
        across(pacc.at[0], *pairs)
        for u, (k, v) in zip(units, pairs):
            q = down(k[...], d_bits)
            qs2[u] = q
            curve = curve + q * v
        return curve

    curve = jnp.zeros((1, local), F32)
    curve = lax.fori_loop(1, FAR // 2, lambda i, c: second(c, 2 * i, 2 * i + 1), curve)
    for u in range(2, FAR):
        to_owner(qs2, qr2, 14, u).start()
    whole(rr, FAR, 16).wait()
    curve = lax.fori_loop(FAR // 2, UNITS // 2, lambda i, c: second(c, 2 * i, 2 * i + 1), curve)
    curve = second(curve, UNITS - 1)
    for u in FAR_UNITS:
        if u >= FAR:
            to_owner(qs2, qr2, 14, u).start()
    applied = row_of() + weight * d_own
    cc[0] = jnp.where(lane == 0, jnp.sum(d_own * applied + curve), 0.0)
    to_all(cc, 4)
    whole(qs2, 2, 14).wait_send()
    whole(qr2, 2, 14).wait_recv()
    applied = applied + jnp.sum(qr2[2:], axis=0)
    whole(cc, 1, 4).wait()
    step1 = norm1 / jnp.sum(jnp.sum(cc[...], axis=0))
    coef_out[...] = step0 * target + step1 * d_own
    res_out[...] = r1 - step1 * applied


def body(points, targets, ridge_weight):
    local, dim = points.shape
    dma = pltpu.SemaphoreType.DMA
    vec = jax.ShapeDtypeStruct((1, local), F32)
    rows = pltpu.VMEM((UNITS, 1, local), F32)
    small = pltpu.VMEM((128, 1, 128), F32)
    chunks = len(CHUNKS)
    coef, res = pl.pallas_call(
        kernel,
        out_shape=(vec, vec),
        in_specs=[
            pl.BlockSpec(memory_space=pl.ANY),
            pl.BlockSpec(memory_space=pltpu.VMEM),
            pl.BlockSpec(memory_space=pltpu.SMEM),
        ],
        out_specs=(pl.BlockSpec(memory_space=pltpu.VMEM), pl.BlockSpec(memory_space=pltpu.VMEM)),
        scratch_shapes=[
            pltpu.VMEM((2, SLOTS, dim, local), BF16),
            pltpu.VMEM((2, SLOTS, 1, 2 * local), F32),
            rows, rows, rows, rows, rows, rows, small, small, small,
            pltpu.VMEM((local, 4 * dim), BF16),
            pltpu.VMEM((2, local, 128), F32),
            pltpu.VMEM((UNITS, local, local), BF16),
            pltpu.VMEM((local, local), BF16),
            pltpu.VMEM((local, local), BF16),
            dma, dma((chunks,)), dma((chunks,)), dma((chunks + 1,)), dma((chunks + 1,)), dma((18,)),
            pltpu.SemaphoreType.REGULAR,
        ],
        compiler_params=pltpu.CompilerParams(
            collective_id=0, has_side_effects=True, vmem_limit_bytes=62 * 1024 * 1024),
    )(points.T, targets.reshape(1, local), ridge_weight.reshape(1, 1))
    return coef.reshape(local), res.reshape(local)


def solution(mesh):
    return jax.shard_map(
        body, mesh=mesh,
        in_specs=(P("pts", None), P("pts"), P()),
        out_specs=(P("pts"), P("pts")), check_vma=False)
```

```python
import jax
import jax.numpy as jnp
from jax import lax
from jax.experimental import pallas as pl
from jax.experimental.pallas import tpu as pltpu
from jax.sharding import PartitionSpec as P

F32 = jnp.float32
BF16 = jnp.bfloat16
TREE = (
    ((0, 0, 1), 0, 2, 1), ((0, 1, 0), 0, 1, 1), ((1, 0, 0), 0, 0, 1), ((1, 3, 0), 3, 1, -1), ((1, 1, 0), 2, 0, 1),
    ((3, 0, 1), 1, 0, -1), ((0, 1, 1), 1, 1, 1), ((0, 1, 3), 2, 2, -1), ((1, 0, 1), 3, 2, 1), ((0, 1, 2), 8, 2, -1),
    ((3, 0, 2), 6, 2, 1), ((1, 1, 1), 5, 2, 1), ((1, 2, 0), 4, 1, -1), ((1, 3, 3), 4, 2, -1), ((2, 0, 1), 6, 0, -1),
    ((2, 3, 0), 4, 0, 1), ((0, 2, 1), 7, 1, 1), ((1, 1, 3), 5, 2, -1), ((1, 3, 1), 9, 1, -1), ((1, 2, 1), 12, 1, 1),
    ((1, 2, 3), 13, 2, -1), ((3, 1, 2), 10, 0, -1), ((2, 3, 1), 15, 1, -1), ((2, 3, 3), 14, 0, 1), ((3, 3, 2), 11, 1, -1),
    ((2, 2, 1), 20, 0, 1), ((1, 2, 2), 21, 2, -1), ((2, 1, 2), 22, 0, -1), ((0, 0, 2), 1, 2, 1), ((0, 2, 0), 2, 1, 1),
    ((2, 0, 0), 3, 0, 1), ((0, 2, 2), 10, 1, 1), ((2, 0, 2), 11, 0, -1), ((2, 2, 0), 16, 1, -1), ((2, 2, 2), 26, 2, 1))
PLACES = ((0, 0, 0),) + tuple(t[0] for t in TREE)
SLOTS = len(PLACES)
SELF = 29
UNITS = 2 * SELF + SLOTS - SELF
CHUNKS = ((1, 3), (4, 6), (10, 10), (20, 6), (26, 3), (29, 3), (32, 3), (35, 1))
LOG2E = 1.4426950408889634


def plane_of(plane, lo, hi):
    return tuple((s, plane) for s in range(lo, hi))


PLAN = (
    ((0,), (), plane_of(0, 1, 4)),
    ((), (0,), plane_of(1, 1, 4)),
    ((1,), (), plane_of(0, 4, 10)),
    ((5,), (1,), plane_of(1, 4, 10)),
    ((2,), (5,), plane_of(0, 10, 16)),
    ((), (), plane_of(0, 16, 20) + plane_of(None, 29, 31)),
    ((3,), (2,), plane_of(1, 10, 16)),
    ((6,), (), plane_of(1, 16, 20) + plane_of(None, 31, 32)),
    ((4,), (), plane_of(0, 20, 26)),
    ((), (3, 6), plane_of(1, 20, 26)),
    ((7,), (4,), plane_of(0, 26, 29) + plane_of(1, 26, 29)),
    ((), (7,), plane_of(None, 32, 36)))
ALL = tuple((z, y, x) for z in range(4) for y in range(4) for x in range(4))


def chunk_of(s):
    return [lo <= s < lo + n for lo, n in CHUNKS].index(True)


def hops(m):
    return sum(min(v, 4 - v) for v in m)


def slot_of(u):
    return (u // 2, u % 2) if u < 2 * SELF else (u - SELF, None)


TOP = 384
WIDTH = 4
FAR = 40
FAR_UNITS = sorted(range(2, UNITS), key=lambda u: -hops(PLACES[slot_of(u)[0]]))
FAR_CHIPS = sorted(ALL, key=lambda m: -hops(m))


def kernel(pts_hbm, tgt_hbm, ridge, coef_out, res_out, tgt, bl, tl, tu, rr, qs1, qr1, qs2, qr2, ca, cb, cc,
           own_l, pacc, kt, ka, kb, sem_in, gb, gt, db, dt, sems, ack):
    me = lax.axis_index("pts")
    local = tgt_hbm.shape[1]
    dim = bl.shape[2]
    half = local // 2
    core = lax.rem(me, 2)
    chip = me // 2
    pos = (chip // 16, lax.rem(chip // 4, 4), lax.rem(chip, 4))
    axis = [[lax.rem(pos[d] + a, 4) * (32, 8, 2)[d] for a in range(4)] for d in range(3)]
    cores = (core, 1 - core)
    upper = [p // 2 for p in pos]

    def device(m, c, sign=1):
        return sum(axis[d][sign * m[d] % 4] for d in range(3)) + c

    def split(s):
        return upper[PLACES[s].index(2)]

    partner = device((0, 0, 0), cores[1])
    load = pltpu.make_async_copy(pts_hbm, bl.at[0, 0], sem_in)
    load.start()
    fetch = pltpu.make_async_copy(tgt_hbm, tgt, sems.at[0])
    fetch.start()
    barrier = pltpu.get_barrier_semaphore()
    near = [partner] + [device(tuple(int(d == i) for i in range(3)), core, sign) for d in range(3) for sign in (1, -1)]
    for dev in near:
        pl.semaphore_signal(barrier, inc=1, device_id=(dev,), device_id_type=pl.DeviceIdType.MESH)

    fetch.wait()
    target = tgt[...]
    t_bits = target.astype(BF16)

    load.wait()
    own_t = bl[0, 0].astype(F32)
    norm_row = jnp.sum(own_t * own_t, axis=0, keepdims=True) * (-LOG2E / dim)
    tl[0, 0] = jnp.concatenate([target, norm_row], axis=1)

    def send(src, dst, ssem, rsem, dev):
        return pltpu.make_async_remote_copy(
            src_ref=src, dst_ref=dst, send_sem=ssem, recv_sem=rsem,
            device_id=(dev,), device_id_type=pl.DeviceIdType.MESH)

    def hop(s):
        _, src, d, sign = TREE[s - 1]
        g = chunk_of(s)
        dev = device(tuple(int(d == i) for i in range(3)), core, sign)
        return (send(bl.at[0, src], bl.at[0, s], sems.at[0], gb.at[g], dev),
                send(tl.at[0, src], tl.at[0, s], sems.at[1], gt.at[g], dev))

    def across_chip(s):
        g = chunk_of(s) if s else len(CHUNKS)
        return (send(bl.at[0, s], bl.at[1, s], sems.at[2], db.at[g], partner),
                send(tl.at[0, s], tl.at[1, s], sems.at[3], dt.at[g], partner))

    def start(copies):
        for copy in copies:
            copy.start()

    def arrive(plane, g):
        lo, n = CHUNKS[g] if g < len(CHUNKS) else (0, 1)
        for buf, sem in ((bl, (gb, db)[plane]), (tl, (gt, dt)[plane])):
            ref = buf.at[plane, pl.ds(lo, n)]
            send(ref, ref, sems.at[0], sem.at[g], partner).wait_recv()

    def serve(g):
        arrive(0, g)
        lo, n = CHUNKS[g]
        for s in range(lo, lo + n):
            start(across_chip(s))
        for s in range(1, SLOTS):
            if lo <= TREE[s - 1][1] < lo + n:
                start(hop(s))
        for s in range(lo, lo + n):
            pl.semaphore_signal(ack, inc=1, device_id=(device(PLACES[s], core, -1),), device_id_type=pl.DeviceIdType.MESH)

    def whole(buf, lo, sem):
        rest = buf.at[pl.ds(lo, buf.shape[0] - lo)]
        return send(rest, rest, sems.at[sem], sems.at[sem + 1], partner)

    def to_owner(qs, qr, sem, u):
        s, plane = slot_of(u)
        c = cores[plane] if plane is not None else lax.rem(core + split(s), 2)
        return send(qs.at[u], qr.at[u], sems.at[sem], sems.at[sem + 1], device(PLACES[s], c, -1))

    def to_user(buf, sem, u):
        s, plane = slot_of(u)
        c = cores[plane] if plane is not None else lax.rem(core + 1 + split(s), 2)
        return send(buf.at[0], buf.at[u], sems.at[sem], sems.at[sem + 1], device(PLACES[s], c))

    def to_all(buf, sem):
        for m in FAR_CHIPS:
            for p in (0, 1):
                if hops(m) + p:
                    at = p * 64 + m[0] * 16 + m[1] * 4 + m[2]
                    send(buf.at[0], buf.at[at], sems.at[sem], sems.at[sem + 1], device(m, cores[p])).start()

    pl.semaphore_wait(barrier, len(near))
    for s in range(1, SLOTS):
        if TREE[s - 1][1] == 0:
            start(hop(s))
    start(across_chip(0))

    def three(x):
        hi = x.astype(BF16).astype(F32)
        mid = (x - hi).astype(BF16).astype(F32)
        return hi, mid, x - hi - mid

    def tagged(lead, then):
        rows = lax.broadcasted_iota(jnp.int32, (8, local), 0)
        out = jnp.zeros((8, local), F32)
        for i, x in enumerate(lead + then):
            out = jnp.where(rows == i, x, out)
        return jnp.concatenate([out, jnp.zeros((8, local), F32)], axis=0)

    ones = (1.0, 1.0, 1.0)
    left = jnp.concatenate([*three(own_t * (2.0 * LOG2E / dim)), tagged(ones, three(norm_row)),
                            jnp.zeros((dim - 16, local), F32)], axis=0)
    own_l[...] = left.T.astype(BF16)
    rest = jnp.zeros((dim - 16, local), BF16)

    def power(u, plane, s):
        row = tl[plane, s]
        tu[u] = row[:, :local]
        pb = bl[plane, s]
        tags = tagged(three(row[:, local:]), ones).astype(BF16)
        right = jnp.concatenate([pb, pb, pb, tags, rest], axis=0)
        return jnp.dot(own_l[...], right, preferred_element_type=F32)

    def keep(u, e, side):
        for r in range(0, local, 32):
            k = jnp.exp2(e[r:r + 32]).astype(BF16)
            kt[u, r:r + 32] = k
            (ka, kb)[side][r:r + 32] = k

    def down(k, bits):
        return jnp.dot(bits, k, preferred_element_type=F32)

    def across(acc, *pairs, rows=None):
        lows = [v.astype(BF16).astype(F32) for _, v in pairs]
        for r in range(0, rows or local, 16):
            cut = pl.ds(r, 16)
            total = acc[cut]
            for (k, _), low in zip(pairs, lows):
                for c in range(0, local, 128):
                    total = total + k[cut, c:c + 128].astype(F32) * low[:, c:c + 128]
            acc[cut] = total

    def row_of():
        return jnp.sum((pacc[0] + pacc[1]).T, axis=0, keepdims=True)

    def absorb(u, side, tw):
        held = (ka, kb)[side]
        v = tu[u]
        q = None
        if u > 1:
            q = down(held[...], t_bits)
            qs1[u] = q
        across(pacc.at[side], (held, v))
        return tw if q is None else tw + q * v

    pacc[...] = jnp.zeros_like(pacc)
    keep(0, power(0, 0, 0), 0)
    across(pacc.at[0], (ka, target))
    arrive(1, len(CHUNKS))
    keep(1, power(1, 1, 0), 1)
    tw = jnp.zeros((1, local), F32)
    sent, ready = [], []

    def send_ready():
        for u in ready:
            to_owner(qs1, qr1, 8, u).start()
        sent.extend(ready)
        ready.clear()

    prev, count = 1, 1
    for served, crossed, units in PLAN:
        for g in served:
            serve(g)
        for g in crossed:
            arrive(1, g)
        send_ready()
        units = [(s + SELF, split(s), s) if plane is None else (2 * s + plane, plane, s) for s, plane in units]
        e = power(*units[0])
        for j, (u, _, _) in enumerate(units):
            ahead = power(*units[j + 1]) if j + 1 < len(units) else None
            tw = absorb(prev, count % 2, tw)
            if prev > 1:
                ready.append(prev)
            count += 1
            keep(u, e, count % 2)
            prev, e = u, ahead

    tw = absorb(prev, count % 2, tw)
    ready.append(prev)

    ready.reverse()
    send_ready()
    weight = ridge[0, 0]
    base = row_of() + weight * target
    lane = lax.broadcasted_iota(jnp.int32, (1, 128), 1)
    ca[0] = jnp.where(lane == 0, jnp.sum(tw + target * base), jnp.where(lane == 1, jnp.sum(target * target), 0.0))
    pl.semaphore_wait(ack, SLOTS - 1)
    to_all(ca, 6)
    moved = bl.at[0, pl.ds(1, SLOTS - 1)], tl.at[0, pl.ds(1, SLOTS - 1)], bl.at[0], tl.at[0]
    for i, ref in enumerate(moved):
        send(ref, ref, sems.at[i], sem_in, partner).wait_send()
    whole(qs1, 2, 8).wait_send()
    whole(qr1, 2, 8).wait_recv()
    w = base + jnp.sum(qr1[2:], axis=0)
    whole(ca, 1, 6).wait()
    sums = jnp.sum(ca[...], axis=0)
    norm0 = jnp.sum(sums[:, 1:2])
    step0 = norm0 / jnp.sum(sums[:, 0:1])
    r1 = target - step0 * w
    rr[0] = r1
    cb[0] = jnp.where(lane == 0, jnp.sum(r1 * r1), 0.0)
    to_all(cb, 12)
    for u in FAR_UNITS:
        to_user(rr, 16 if u >= FAR else 10, u).start()
    send(rr.at[0], rr.at[1], sems.at[10], sems.at[11], partner).start()
    whole(cb, 1, 12).wait()
    norm1 = jnp.sum(jnp.sum(cb[...], axis=0))
    beta = norm1 / norm0
    whole(rr.at[pl.ds(0, FAR)], 1, 10).wait()

    d_own = r1 + beta * target
    d_bits = d_own.astype(BF16)
    pacc[...] = jnp.zeros_like(pacc)

    def again(u):
        return kt.at[u], rr[u] + beta * tu[u]

    across(pacc.at[0], again(0), again(1))

    def second(carry, *units):
        curve, tail = carry
        pairs = [again(u) for u in units]
        for k, v in pairs:
            tail = tail + lax.dot_general(v.astype(BF16), k[TOP:], (((1,), (1,)), ((), ())), preferred_element_type=F32)
        across(pacc.at[0], *pairs, rows=TOP)
        for u, (k, v) in zip(units, pairs):
            q = down(k[...], d_bits)
            qs2[u] = q
            curve = curve + q * v
        return curve, tail

    def seconds(carry, lo, hi):
        steps = (hi - lo) // WIDTH
        carry = lax.fori_loop(0, steps, lambda i, c: second(c, *(lo + WIDTH * i + j for j in range(WIDTH))), carry)
        rest = range(lo + WIDTH * steps, hi)
        return second(carry, *rest) if rest else carry

    carry = (jnp.zeros((1, local), F32), jnp.zeros((1, local - TOP), F32))
    carry = seconds(carry, 2, FAR)
    for u in range(2, FAR):
        to_owner(qs2, qr2, 14, u).start()
    whole(rr, FAR, 16).wait()
    curve, tail = seconds(carry, FAR, UNITS)
    for u in FAR_UNITS:
        if u >= FAR:
            to_owner(qs2, qr2, 14, u).start()
    applied = row_of() + jnp.concatenate([jnp.zeros((1, TOP), F32), tail], axis=1) + weight * d_own
    cc[0] = jnp.where(lane == 0, jnp.sum(d_own * applied + curve), 0.0)
    to_all(cc, 4)
    whole(qs2, 2, 14).wait_send()
    whole(qr2, 2, 14).wait_recv()
    applied = applied + jnp.sum(qr2[2:], axis=0)
    whole(cc, 1, 4).wait()
    step1 = norm1 / jnp.sum(jnp.sum(cc[...], axis=0))
    coef_out[...] = (step0 * target + step1 * d_own).reshape(local)
    res_out[...] = (r1 - step1 * applied).reshape(local)


def body(points, targets, ridge_weight):
    local, dim = points.shape
    dma = pltpu.SemaphoreType.DMA
    vec = jax.ShapeDtypeStruct((local,), F32)
    rows = pltpu.VMEM((UNITS, 1, local), F32)
    small = pltpu.VMEM((128, 1, 128), F32)
    chunks = len(CHUNKS)
    coef, res = pl.pallas_call(
        kernel,
        out_shape=(vec, vec),
        in_specs=[
            pl.BlockSpec(memory_space=pl.ANY),
            pl.BlockSpec(memory_space=pl.ANY),
            pl.BlockSpec(memory_space=pltpu.SMEM),
        ],
        out_specs=(pl.BlockSpec(memory_space=pltpu.VMEM), pl.BlockSpec(memory_space=pltpu.VMEM)),
        scratch_shapes=[
            pltpu.VMEM((1, local), F32),
            pltpu.VMEM((2, SLOTS, dim, local), BF16),
            pltpu.VMEM((2, SLOTS, 1, 2 * local), F32),
            rows, rows, rows, rows, rows, rows, small, small, small,
            pltpu.VMEM((local, 4 * dim), BF16),
            pltpu.VMEM((2, local, 128), F32),
            pltpu.VMEM((UNITS, local, local), BF16),
            pltpu.VMEM((local, local), BF16),
            pltpu.VMEM((local, local), BF16),
            dma, dma((chunks,)), dma((chunks,)), dma((chunks + 1,)), dma((chunks + 1,)), dma((18,)),
            pltpu.SemaphoreType.REGULAR,
        ],
        compiler_params=pltpu.CompilerParams(
            collective_id=0, has_side_effects=True, vmem_limit_bytes=62 * 1024 * 1024),
    )(points.T, targets.reshape(1, local), ridge_weight.reshape(1, 1))
    return coef, res


def solution(mesh):
    return jax.shard_map(
        body, mesh=mesh,
        in_specs=(P("pts", None), P("pts"), P()),
        out_specs=(P("pts"), P("pts")), check_vma=False)
```

```python
import jax
import jax.numpy as jnp
from jax import lax
from jax.experimental import pallas as pl
from jax.experimental.pallas import tpu as pltpu
from jax.sharding import PartitionSpec as P

F32 = jnp.float32
BF16 = jnp.bfloat16
TREE = (
    ((0, 0, 1), 0, 2, 1), ((0, 1, 0), 0, 1, 1), ((1, 0, 0), 0, 0, 1), ((1, 3, 0), 3, 1, -1), ((1, 1, 0), 2, 0, 1),
    ((3, 0, 1), 1, 0, -1), ((0, 1, 1), 1, 1, 1), ((0, 1, 3), 2, 2, -1), ((1, 0, 1), 3, 2, 1), ((0, 1, 2), 8, 2, -1),
    ((3, 0, 2), 6, 2, 1), ((1, 1, 1), 5, 2, 1), ((1, 2, 0), 4, 1, -1), ((1, 3, 3), 4, 2, -1), ((2, 0, 1), 6, 0, -1),
    ((2, 3, 0), 4, 0, 1), ((0, 2, 1), 7, 1, 1), ((1, 1, 3), 5, 2, -1), ((1, 3, 1), 9, 1, -1), ((1, 2, 1), 12, 1, 1),
    ((1, 2, 3), 13, 2, -1), ((3, 1, 2), 10, 0, -1), ((2, 3, 1), 15, 1, -1), ((2, 3, 3), 14, 0, 1), ((3, 3, 2), 11, 1, -1),
    ((2, 2, 1), 20, 0, 1), ((1, 2, 2), 21, 2, -1), ((2, 1, 2), 22, 0, -1), ((0, 0, 2), 1, 2, 1), ((0, 2, 0), 2, 1, 1),
    ((2, 0, 0), 3, 0, 1), ((0, 2, 2), 10, 1, 1), ((2, 0, 2), 11, 0, -1), ((2, 2, 0), 16, 1, -1), ((2, 2, 2), 26, 2, 1))
PLACES = ((0, 0, 0),) + tuple(t[0] for t in TREE)
SLOTS = len(PLACES)
SELF = 29
UNITS = 2 * SELF + SLOTS - SELF
CHUNKS = ((1, 3), (4, 6), (10, 10), (20, 6), (26, 3), (29, 3), (32, 3), (35, 1))
LOG2E = 1.4426950408889634


def plane_of(plane, lo, hi):
    return tuple((s, plane) for s in range(lo, hi))


PLAN = (
    ((0,), (), plane_of(0, 1, 4)),
    ((), (0,), plane_of(1, 1, 4)),
    ((1,), (), plane_of(0, 4, 10)),
    ((5,), (1,), plane_of(1, 4, 10)),
    ((2,), (5,), plane_of(0, 10, 16)),
    ((), (), plane_of(0, 16, 20) + plane_of(None, 29, 31)),
    ((3,), (2,), plane_of(1, 10, 16)),
    ((6,), (), plane_of(1, 16, 20) + plane_of(None, 31, 32)),
    ((4,), (), plane_of(0, 20, 26)),
    ((), (3, 6), plane_of(1, 20, 26)),
    ((7,), (4,), plane_of(0, 26, 29) + plane_of(1, 26, 29)),
    ((), (7,), plane_of(None, 32, 36)))
ALL = tuple((z, y, x) for z in range(4) for y in range(4) for x in range(4))


def chunk_of(s):
    return [lo <= s < lo + n for lo, n in CHUNKS].index(True)


def hops(m):
    return sum(min(v, 4 - v) for v in m)


def slot_of(u):
    return (u // 2, u % 2) if u < 2 * SELF else (u - SELF, None)


TOP = 384
WIDTH = 4
FAR = 40
FAR_UNITS = sorted(range(2, UNITS), key=lambda u: -hops(PLACES[slot_of(u)[0]]))
FAR_CHIPS = sorted(ALL, key=lambda m: -hops(m))


def kernel(pts_hbm, tgt_hbm, ridge, coef_out, res_out, tgt, bl, tl, tu, rr, qs1, qr1, qs2, qr2, ca, cb, cc,
           own_l, pacc, kt, ka, kb, sem_in, gb, gt, db, dt, sems, ack):
    me = lax.axis_index("pts")
    local = tgt_hbm.shape[1]
    dim = bl.shape[2]
    half = local // 2
    core = lax.rem(me, 2)
    chip = me // 2
    pos = (chip // 16, lax.rem(chip // 4, 4), lax.rem(chip, 4))
    axis = [[lax.rem(pos[d] + a, 4) * (32, 8, 2)[d] for a in range(4)] for d in range(3)]
    cores = (core, 1 - core)
    upper = [p // 2 for p in pos]

    def device(m, c, sign=1):
        return sum(axis[d][sign * m[d] % 4] for d in range(3)) + c

    def split(s):
        return upper[PLACES[s].index(2)]

    partner = device((0, 0, 0), cores[1])
    load = pltpu.make_async_copy(pts_hbm, bl.at[0, 0], sem_in)
    load.start()
    fetch = pltpu.make_async_copy(tgt_hbm, tgt, sems.at[0])
    fetch.start()
    barrier = pltpu.get_barrier_semaphore()
    near = [partner] + [device(tuple(int(d == i) for i in range(3)), core, sign) for d in range(3) for sign in (1, -1)]
    for dev in near:
        pl.semaphore_signal(barrier, inc=1, device_id=(dev,), device_id_type=pl.DeviceIdType.MESH)

    fetch.wait()
    target = tgt[...]
    t_bits = target.astype(BF16)

    load.wait()
    own_t = bl[0, 0].astype(F32)
    norm_row = jnp.sum(own_t * own_t, axis=0, keepdims=True) * (-LOG2E / dim)
    tl[0, 0] = jnp.concatenate([target, norm_row], axis=1)

    def send(src, dst, ssem, rsem, dev):
        return pltpu.make_async_remote_copy(
            src_ref=src, dst_ref=dst, send_sem=ssem, recv_sem=rsem,
            device_id=(dev,), device_id_type=pl.DeviceIdType.MESH)

    def hop(s):
        _, src, d, sign = TREE[s - 1]
        g = chunk_of(s)
        dev = device(tuple(int(d == i) for i in range(3)), core, sign)
        return (send(bl.at[0, src], bl.at[0, s], sems.at[0], gb.at[g], dev),
                send(tl.at[0, src], tl.at[0, s], sems.at[1], gt.at[g], dev))

    def across_chip(s):
        g = chunk_of(s) if s else len(CHUNKS)
        return (send(bl.at[0, s], bl.at[1, s], sems.at[2], db.at[g], partner),
                send(tl.at[0, s], tl.at[1, s], sems.at[3], dt.at[g], partner))

    def start(copies):
        for copy in copies:
            copy.start()

    def arrive(plane, g):
        lo, n = CHUNKS[g] if g < len(CHUNKS) else (0, 1)
        for buf, sem in ((bl, (gb, db)[plane]), (tl, (gt, dt)[plane])):
            ref = buf.at[plane, pl.ds(lo, n)]
            send(ref, ref, sems.at[0], sem.at[g], partner).wait_recv()

    def serve(g):
        arrive(0, g)
        lo, n = CHUNKS[g]
        for s in range(lo, lo + n):
            start(across_chip(s))
        for s in range(1, SLOTS):
            if lo <= TREE[s - 1][1] < lo + n:
                start(hop(s))
        for s in range(lo, min(lo + n, SELF)):
            pl.semaphore_signal(ack, inc=1, device_id=(device(PLACES[s], core, -1),), device_id_type=pl.DeviceIdType.MESH)

    def whole(buf, lo, sem):
        rest = buf.at[pl.ds(lo, buf.shape[0] - lo)]
        return send(rest, rest, sems.at[sem], sems.at[sem + 1], partner)

    def to_owner(qs, qr, sem, u):
        s, plane = slot_of(u)
        c = cores[plane] if plane is not None else lax.rem(core + split(s), 2)
        return send(qs.at[u], qr.at[u], sems.at[sem], sems.at[sem + 1], device(PLACES[s], c, -1))

    def to_user(buf, sem, u):
        s, plane = slot_of(u)
        c = cores[plane] if plane is not None else lax.rem(core + 1 + split(s), 2)
        return send(buf.at[0], buf.at[u], sems.at[sem], sems.at[sem + 1], device(PLACES[s], c))

    def to_all(buf, sem):
        for m in FAR_CHIPS:
            for p in (0, 1):
                if hops(m) + p:
                    at = p * 64 + m[0] * 16 + m[1] * 4 + m[2]
                    send(buf.at[0], buf.at[at], sems.at[sem], sems.at[sem + 1], device(m, cores[p])).start()

    pl.semaphore_wait(barrier, len(near))
    for s in range(1, SLOTS):
        if TREE[s - 1][1] == 0:
            start(hop(s))
    start(across_chip(0))

    def three(x):
        hi = x.astype(BF16).astype(F32)
        mid = (x - hi).astype(BF16).astype(F32)
        return hi, mid, x - hi - mid

    def tagged(lead, then):
        rows = lax.broadcasted_iota(jnp.int32, (8, local), 0)
        out = jnp.zeros((8, local), F32)
        for i, x in enumerate(lead + then):
            out = jnp.where(rows == i, x, out)
        return jnp.concatenate([out, jnp.zeros((8, local), F32)], axis=0)

    ones = (1.0, 1.0, 1.0)
    left = jnp.concatenate([*three(own_t * (2.0 * LOG2E / dim)), tagged(ones, three(norm_row)),
                            jnp.zeros((dim - 16, local), F32)], axis=0)
    own_l[...] = left.T.astype(BF16)
    rest = jnp.zeros((dim - 16, local), BF16)

    def power(u, plane, s):
        row = tl[plane, s]
        tu[u] = row[:, :local]
        pb = bl[plane, s]
        tags = tagged(three(row[:, local:]), ones).astype(BF16)
        right = jnp.concatenate([pb, pb, pb, tags, rest], axis=0)
        return jnp.dot(own_l[...], right, preferred_element_type=F32)

    def keep(u, e, side):
        for r in range(0, local, 32):
            k = jnp.exp2(e[r:r + 32]).astype(BF16)
            kt[u, r:r + 32] = k
            (ka, kb)[side][r:r + 32] = k

    def down(k, bits):
        return jnp.dot(bits, k, preferred_element_type=F32)

    def across(acc, *pairs, rows=None):
        lows = [v.astype(BF16).astype(F32) for _, v in pairs]
        for r in range(0, rows or local, 16):
            cut = pl.ds(r, 16)
            total = acc[cut]
            for (k, _), low in zip(pairs, lows):
                for c in range(0, local, 128):
                    total = total + k[cut, c:c + 128].astype(F32) * low[:, c:c + 128]
            acc[cut] = total

    def row_of():
        return jnp.sum((pacc[0] + pacc[1]).T, axis=0, keepdims=True)

    def absorb(u, side, tw):
        held = (ka, kb)[side]
        v = tu[u]
        q = None
        if u > 1:
            q = down(held[...], t_bits)
            qs1[u] = q
        across(pacc.at[side], (held, v))
        return tw if q is None else tw + q * v

    pacc[...] = jnp.zeros_like(pacc)
    keep(0, power(0, 0, 0), 0)
    across(pacc.at[0], (ka, target))
    arrive(1, len(CHUNKS))
    keep(1, power(1, 1, 0), 1)
    tw = jnp.zeros((1, local), F32)
    sent, ready = [], []

    def send_ready():
        for u in ready:
            to_owner(qs1, qr1, 8, u).start()
        sent.extend(ready)
        ready.clear()

    prev, count = 1, 1
    for served, crossed, units in PLAN:
        for g in served:
            serve(g)
        for g in crossed:
            arrive(1, g)
        send_ready()
        units = [(s + SELF, split(s), s) if plane is None else (2 * s + plane, plane, s) for s, plane in units]
        e = power(*units[0])
        for j, (u, _, _) in enumerate(units):
            ahead = power(*units[j + 1]) if j + 1 < len(units) else None
            tw = absorb(prev, count % 2, tw)
            if prev > 1:
                ready.append(prev)
            count += 1
            keep(u, e, count % 2)
            prev, e = u, ahead

    tw = absorb(prev, count % 2, tw)
    ready.append(prev)

    ready.reverse()
    send_ready()
    weight = ridge[0, 0]
    base = row_of() + weight * target
    lane = lax.broadcasted_iota(jnp.int32, (1, 128), 1)
    ca[0] = jnp.where(lane == 0, jnp.sum(tw + target * base), jnp.where(lane == 1, jnp.sum(target * target), 0.0))
    pl.semaphore_wait(ack, SELF - 1)
    to_all(ca, 6)
    moved = bl.at[0, pl.ds(1, SLOTS - 1)], tl.at[0, pl.ds(1, SLOTS - 1)], bl.at[0], tl.at[0]
    for i, ref in enumerate(moved):
        send(ref, ref, sems.at[i], sem_in, partner).wait_send()
    whole(qs1, 2, 8).wait_send()
    whole(qr1, 2, 8).wait_recv()
    w = base + jnp.sum(qr1[2:], axis=0)
    whole(ca, 1, 6).wait()
    sums = jnp.sum(ca[...], axis=0)
    norm0 = jnp.sum(sums[:, 1:2])
    step0 = norm0 / jnp.sum(sums[:, 0:1])
    r1 = target - step0 * w
    rr[0] = r1
    cb[0] = jnp.where(lane == 0, jnp.sum(r1 * r1), 0.0)
    to_all(cb, 12)
    for u in FAR_UNITS:
        to_user(rr, 16 if u >= FAR else 10, u).start()
    send(rr.at[0], rr.at[1], sems.at[10], sems.at[11], partner).start()
    whole(cb, 1, 12).wait()
    norm1 = jnp.sum(jnp.sum(cb[...], axis=0))
    beta = norm1 / norm0
    whole(rr.at[pl.ds(0, FAR)], 1, 10).wait()

    d_own = r1 + beta * target
    d_bits = d_own.astype(BF16)
    pacc[...] = jnp.zeros_like(pacc)

    def again(u):
        return kt.at[u], rr[u] + beta * tu[u]

    across(pacc.at[0], again(0), again(1))

    def second(carry, *units):
        curve, tail = carry
        pairs = [again(u) for u in units]
        for k, v in pairs:
            tail = tail + lax.dot_general(v.astype(BF16), k[TOP:], (((1,), (1,)), ((), ())), preferred_element_type=F32)
        across(pacc.at[0], *pairs, rows=TOP)
        for u, (k, v) in zip(units, pairs):
            q = down(k[...], d_bits)
            qs2[u] = q
            curve = curve + q * v
        return curve, tail

    def seconds(carry, lo, hi):
        steps = (hi - lo) // WIDTH
        carry = lax.fori_loop(0, steps, lambda i, c: second(c, *(lo + WIDTH * i + j for j in range(WIDTH))), carry)
        rest = range(lo + WIDTH * steps, hi)
        return second(carry, *rest) if rest else carry

    carry = (jnp.zeros((1, local), F32), jnp.zeros((1, local - TOP), F32))
    carry = seconds(carry, 2, FAR)
    for u in range(2, FAR):
        to_owner(qs2, qr2, 14, u).start()
    whole(rr, FAR, 16).wait()
    curve, tail = seconds(carry, FAR, UNITS)
    for u in FAR_UNITS:
        if u >= FAR:
            to_owner(qs2, qr2, 14, u).start()
    applied = row_of() + jnp.concatenate([jnp.zeros((1, TOP), F32), tail], axis=1) + weight * d_own
    cc[0] = jnp.where(lane == 0, jnp.sum(d_own * applied + curve), 0.0)
    to_all(cc, 4)
    whole(qs2, 2, 14).wait_send()
    whole(qr2, 2, 14).wait_recv()
    applied = applied + jnp.sum(qr2[2:], axis=0)
    whole(cc, 1, 4).wait()
    step1 = norm1 / jnp.sum(jnp.sum(cc[...], axis=0))
    coef_out[...] = (step0 * target + step1 * d_own).reshape(local)
    res_out[...] = (r1 - step1 * applied).reshape(local)


def body(points, targets, ridge_weight):
    local, dim = points.shape
    dma = pltpu.SemaphoreType.DMA
    vec = jax.ShapeDtypeStruct((local,), F32)
    rows = pltpu.VMEM((UNITS, 1, local), F32)
    small = pltpu.VMEM((128, 1, 128), F32)
    chunks = len(CHUNKS)
    coef, res = pl.pallas_call(
        kernel,
        out_shape=(vec, vec),
        in_specs=[
            pl.BlockSpec(memory_space=pl.ANY),
            pl.BlockSpec(memory_space=pl.ANY),
            pl.BlockSpec(memory_space=pltpu.SMEM),
        ],
        out_specs=(pl.BlockSpec(memory_space=pltpu.VMEM), pl.BlockSpec(memory_space=pltpu.VMEM)),
        scratch_shapes=[
            pltpu.VMEM((1, local), F32),
            pltpu.VMEM((2, SLOTS, dim, local), BF16),
            pltpu.VMEM((2, SLOTS, 1, 2 * local), F32),
            rows, rows, rows, rows, rows, rows, small, small, small,
            pltpu.VMEM((local, 4 * dim), BF16),
            pltpu.VMEM((2, local, 128), F32),
            pltpu.VMEM((UNITS, local, local), BF16),
            pltpu.VMEM((local, local), BF16),
            pltpu.VMEM((local, local), BF16),
            dma, dma((chunks,)), dma((chunks,)), dma((chunks + 1,)), dma((chunks + 1,)), dma((18,)),
            pltpu.SemaphoreType.REGULAR,
        ],
        compiler_params=pltpu.CompilerParams(
            collective_id=0, has_side_effects=True, vmem_limit_bytes=62 * 1024 * 1024),
    )(points.T, targets.reshape(1, local), ridge_weight.reshape(1, 1))
    return coef, res


def solution(mesh):
    return jax.shard_map(
        body, mesh=mesh,
        in_specs=(P("pts", None), P("pts"), P()),
        out_specs=(P("pts"), P("pts")), check_vma=False)
```

```python
import jax
import jax.numpy as jnp
from jax import lax
from jax.experimental import pallas as pl
from jax.experimental.pallas import tpu as pltpu
from jax.sharding import PartitionSpec as P

F32 = jnp.float32
BF16 = jnp.bfloat16
TREE = (
    ((0, 0, 1), 0, 2, 1), ((0, 1, 0), 0, 1, 1), ((1, 0, 0), 0, 0, 1), ((1, 3, 0), 3, 1, -1), ((1, 1, 0), 2, 0, 1),
    ((3, 0, 1), 1, 0, -1), ((0, 1, 1), 1, 1, 1), ((0, 1, 3), 2, 2, -1), ((1, 0, 1), 3, 2, 1), ((0, 1, 2), 8, 2, -1),
    ((3, 0, 2), 6, 2, 1), ((1, 1, 1), 5, 2, 1), ((1, 2, 0), 4, 1, -1), ((1, 3, 3), 4, 2, -1), ((2, 0, 1), 6, 0, -1),
    ((2, 3, 0), 4, 0, 1), ((0, 2, 1), 7, 1, 1), ((1, 1, 3), 5, 2, -1), ((1, 3, 1), 9, 1, -1), ((1, 2, 1), 12, 1, 1),
    ((1, 2, 3), 13, 2, -1), ((3, 1, 2), 10, 0, -1), ((2, 3, 1), 15, 1, -1), ((2, 3, 3), 14, 0, 1), ((3, 3, 2), 11, 1, -1),
    ((2, 2, 1), 20, 0, 1), ((1, 2, 2), 21, 2, -1), ((2, 1, 2), 22, 0, -1), ((0, 0, 2), 1, 2, 1), ((0, 2, 0), 2, 1, 1),
    ((2, 0, 0), 3, 0, 1), ((0, 2, 2), 10, 1, 1), ((2, 0, 2), 11, 0, -1), ((2, 2, 0), 16, 1, -1), ((2, 2, 2), 26, 2, 1))
PLACES = ((0, 0, 0),) + tuple(t[0] for t in TREE)
SLOTS = len(PLACES)
SELF = 29
UNITS = 2 * SELF + SLOTS - SELF
CHUNKS = ((1, 3), (4, 6), (10, 10), (20, 6), (26, 3), (29, 3), (32, 3), (35, 1))
LOG2E = 1.4426950408889634


def plane_of(plane, lo, hi):
    return tuple((s, plane) for s in range(lo, hi))


PLAN = (
    ((0,), (), plane_of(0, 1, 4)),
    ((), (0,), plane_of(1, 1, 4)),
    ((1,), (), plane_of(0, 4, 10)),
    ((5,), (1,), plane_of(1, 4, 10)),
    ((2,), (5,), plane_of(0, 10, 16)),
    ((), (), plane_of(0, 16, 20) + plane_of(None, 29, 31)),
    ((3,), (2,), plane_of(1, 10, 16)),
    ((6,), (), plane_of(1, 16, 20) + plane_of(None, 31, 32)),
    ((4,), (), plane_of(0, 20, 26)),
    ((), (3, 6), plane_of(1, 20, 26)),
    ((7,), (), plane_of(0, 26, 29) + plane_of(None, 32, 35)),
    ((), (4,), plane_of(1, 26, 29)),
    ((), (7,), plane_of(None, 35, 36)))
ALL = tuple((z, y, x) for z in range(4) for y in range(4) for x in range(4))


def chunk_of(s):
    return [lo <= s < lo + n for lo, n in CHUNKS].index(True)


def hops(m):
    return sum(min(v, 4 - v) for v in m)


def slot_of(u):
    return (u // 2, u % 2) if u < 2 * SELF else (u - SELF, None)


TOP = 384
WIDTH = 4
FAR = 40
FAR_UNITS = sorted(range(2, UNITS), key=lambda u: -hops(PLACES[slot_of(u)[0]]))
FAR_CHIPS = sorted(ALL, key=lambda m: -hops(m))


def kernel(pts_hbm, tgt_hbm, ridge, coef_out, res_out, tgt, bl, tl, tu, rr, qs1, qr1, qs2, qr2, ca, cb, cc,
           own_l, pacc, kt, ka, kb, sem_in, gb, gt, db, dt, sems, ack):
    me = lax.axis_index("pts")
    local = tgt_hbm.shape[1]
    dim = bl.shape[2]
    half = local // 2
    core = lax.rem(me, 2)
    chip = me // 2
    pos = (chip // 16, lax.rem(chip // 4, 4), lax.rem(chip, 4))
    axis = [[lax.rem(pos[d] + a, 4) * (32, 8, 2)[d] for a in range(4)] for d in range(3)]
    cores = (core, 1 - core)
    upper = [p // 2 for p in pos]

    def device(m, c, sign=1):
        return sum(axis[d][sign * m[d] % 4] for d in range(3)) + c

    def split(s):
        return upper[PLACES[s].index(2)]

    partner = device((0, 0, 0), cores[1])
    load = pltpu.make_async_copy(pts_hbm, bl.at[0, 0], sem_in)
    load.start()
    fetch = pltpu.make_async_copy(tgt_hbm, tgt, sems.at[0])
    fetch.start()
    barrier = pltpu.get_barrier_semaphore()
    near = [partner] + [device(tuple(int(d == i) for i in range(3)), core, sign) for d in range(3) for sign in (1, -1)]
    for dev in near:
        pl.semaphore_signal(barrier, inc=1, device_id=(dev,), device_id_type=pl.DeviceIdType.MESH)

    fetch.wait()
    target = tgt[...]
    t_bits = target.astype(BF16)

    load.wait()
    own_t = bl[0, 0].astype(F32)
    norm_row = jnp.sum(own_t * own_t, axis=0, keepdims=True) * (-LOG2E / dim)
    tl[0, 0] = jnp.concatenate([target, norm_row], axis=1)

    def send(src, dst, ssem, rsem, dev):
        return pltpu.make_async_remote_copy(
            src_ref=src, dst_ref=dst, send_sem=ssem, recv_sem=rsem,
            device_id=(dev,), device_id_type=pl.DeviceIdType.MESH)

    def hop(s):
        _, src, d, sign = TREE[s - 1]
        g = chunk_of(s)
        dev = device(tuple(int(d == i) for i in range(3)), core, sign)
        return (send(bl.at[0, src], bl.at[0, s], sems.at[0], gb.at[g], dev),
                send(tl.at[0, src], tl.at[0, s], sems.at[1], gt.at[g], dev))

    def across_chip(s):
        g = chunk_of(s) if s else len(CHUNKS)
        return (send(bl.at[0, s], bl.at[1, s], sems.at[2], db.at[g], partner),
                send(tl.at[0, s], tl.at[1, s], sems.at[3], dt.at[g], partner))

    def start(copies):
        for copy in copies:
            copy.start()

    def arrive(plane, g):
        lo, n = CHUNKS[g] if g < len(CHUNKS) else (0, 1)
        for buf, sem in ((bl, (gb, db)[plane]), (tl, (gt, dt)[plane])):
            ref = buf.at[plane, pl.ds(lo, n)]
            send(ref, ref, sems.at[0], sem.at[g], partner).wait_recv()

    def serve(g):
        arrive(0, g)
        lo, n = CHUNKS[g]
        for s in range(lo, lo + n):
            start(across_chip(s))
        for s in range(1, SLOTS):
            if lo <= TREE[s - 1][1] < lo + n:
                start(hop(s))
        for s in range(lo, min(lo + n, SELF)):
            pl.semaphore_signal(ack, inc=1, device_id=(device(PLACES[s], core, -1),), device_id_type=pl.DeviceIdType.MESH)

    def whole(buf, lo, sem):
        rest = buf.at[pl.ds(lo, buf.shape[0] - lo)]
        return send(rest, rest, sems.at[sem], sems.at[sem + 1], partner)

    def to_owner(qs, qr, sem, u):
        s, plane = slot_of(u)
        c = cores[plane] if plane is not None else lax.rem(core + split(s), 2)
        return send(qs.at[u], qr.at[u], sems.at[sem], sems.at[sem + 1], device(PLACES[s], c, -1))

    def to_user(buf, sem, u):
        s, plane = slot_of(u)
        c = cores[plane] if plane is not None else lax.rem(core + 1 + split(s), 2)
        return send(buf.at[0], buf.at[u], sems.at[sem], sems.at[sem + 1], device(PLACES[s], c))

    def to_all(buf, sem):
        for m in FAR_CHIPS:
            for p in (0, 1):
                if hops(m) + p:
                    at = p * 64 + m[0] * 16 + m[1] * 4 + m[2]
                    send(buf.at[0], buf.at[at], sems.at[sem], sems.at[sem + 1], device(m, cores[p])).start()

    pl.semaphore_wait(barrier, len(near))
    for s in range(1, SLOTS):
        if TREE[s - 1][1] == 0:
            start(hop(s))
    start(across_chip(0))

    def three(x):
        hi = x.astype(BF16).astype(F32)
        mid = (x - hi).astype(BF16).astype(F32)
        return hi, mid, x - hi - mid

    def tagged(lead, then):
        rows = lax.broadcasted_iota(jnp.int32, (8, local), 0)
        out = jnp.zeros((8, local), F32)
        for i, x in enumerate(lead + then):
            out = jnp.where(rows == i, x, out)
        return jnp.concatenate([out, jnp.zeros((8, local), F32)], axis=0)

    ones = (1.0, 1.0, 1.0)
    left = jnp.concatenate([*three(own_t * (2.0 * LOG2E / dim)), tagged(ones, three(norm_row)),
                            jnp.zeros((dim - 16, local), F32)], axis=0)
    own_l[...] = left.T.astype(BF16)
    rest = jnp.zeros((dim - 16, local), BF16)

    def power(u, plane, s):
        row = tl[plane, s]
        tu[u] = row[:, :local]
        pb = bl[plane, s]
        tags = tagged(three(row[:, local:]), ones).astype(BF16)
        right = jnp.concatenate([pb, pb, pb, tags, rest], axis=0)
        return jnp.dot(own_l[...], right, preferred_element_type=F32)

    def keep(u, e, side):
        for r in range(0, local, 32):
            k = jnp.exp2(e[r:r + 32]).astype(BF16)
            kt[u, r:r + 32] = k
            (ka, kb)[side][r:r + 32] = k

    def down(k, bits):
        return jnp.dot(bits, k, preferred_element_type=F32)

    def across(acc, *pairs, rows=None):
        lows = [v.astype(BF16).astype(F32) for _, v in pairs]
        for r in range(0, rows or local, 16):
            cut = pl.ds(r, 16)
            total = acc[cut]
            for (k, _), low in zip(pairs, lows):
                for c in range(0, local, 128):
                    total = total + k[cut, c:c + 128].astype(F32) * low[:, c:c + 128]
            acc[cut] = total

    def row_of():
        return jnp.sum((pacc[0] + pacc[1]).T, axis=0, keepdims=True)

    def absorb(u, side, tw):
        held = (ka, kb)[side]
        v = tu[u]
        q = None
        if u > 1:
            q = down(held[...], t_bits)
            qs1[u] = q
        across(pacc.at[side], (held, v))
        return tw if q is None else tw + q * v

    pacc[...] = jnp.zeros_like(pacc)
    keep(0, power(0, 0, 0), 0)
    across(pacc.at[0], (ka, target))
    arrive(1, len(CHUNKS))
    keep(1, power(1, 1, 0), 1)
    tw = jnp.zeros((1, local), F32)
    sent, ready = [], []

    def send_ready():
        for u in ready:
            to_owner(qs1, qr1, 8, u).start()
        sent.extend(ready)
        ready.clear()

    prev, count = 1, 1
    for served, crossed, units in PLAN:
        for g in served:
            serve(g)
        for g in crossed:
            arrive(1, g)
        send_ready()
        units = [(s + SELF, split(s), s) if plane is None else (2 * s + plane, plane, s) for s, plane in units]
        e = power(*units[0])
        for j, (u, _, _) in enumerate(units):
            ahead = power(*units[j + 1]) if j + 1 < len(units) else None
            tw = absorb(prev, count % 2, tw)
            if prev > 1:
                ready.append(prev)
            count += 1
            keep(u, e, count % 2)
            prev, e = u, ahead

    tw = absorb(prev, count % 2, tw)
    ready.append(prev)

    ready.reverse()
    send_ready()
    weight = ridge[0, 0]
    base = row_of() + weight * target
    lane = lax.broadcasted_iota(jnp.int32, (1, 128), 1)
    ca[0] = jnp.where(lane == 0, jnp.sum(tw + target * base), jnp.where(lane == 1, jnp.sum(target * target), 0.0))
    pl.semaphore_wait(ack, SELF - 1)
    to_all(ca, 6)
    moved = bl.at[0, pl.ds(1, SLOTS - 1)], tl.at[0, pl.ds(1, SLOTS - 1)], bl.at[0], tl.at[0]
    for i, ref in enumerate(moved):
        send(ref, ref, sems.at[i], sem_in, partner).wait_send()
    whole(qs1, 2, 8).wait_send()
    whole(qr1, 2, 8).wait_recv()
    w = base + jnp.sum(qr1[2:], axis=0)
    whole(ca, 1, 6).wait()
    sums = jnp.sum(ca[...], axis=0)
    norm0 = jnp.sum(sums[:, 1:2])
    step0 = norm0 / jnp.sum(sums[:, 0:1])
    r1 = target - step0 * w
    rr[0] = r1
    cb[0] = jnp.where(lane == 0, jnp.sum(r1 * r1), 0.0)
    to_all(cb, 12)
    for u in FAR_UNITS:
        to_user(rr, 16 if u >= FAR else 10, u).start()
    send(rr.at[0], rr.at[1], sems.at[10], sems.at[11], partner).start()
    whole(cb, 1, 12).wait()
    norm1 = jnp.sum(jnp.sum(cb[...], axis=0))
    beta = norm1 / norm0
    whole(rr.at[pl.ds(0, FAR)], 1, 10).wait()

    d_own = r1 + beta * target
    d_bits = d_own.astype(BF16)
    pacc[...] = jnp.zeros_like(pacc)

    def again(u):
        return kt.at[u], rr[u] + beta * tu[u]

    across(pacc.at[0], again(0), again(1))

    def second(carry, *units):
        curve, tail = carry
        pairs = [again(u) for u in units]
        for k, v in pairs:
            tail = tail + lax.dot_general(v.astype(BF16), k[TOP:], (((1,), (1,)), ((), ())), preferred_element_type=F32)
        across(pacc.at[0], *pairs, rows=TOP)
        for u, (k, v) in zip(units, pairs):
            q = down(k[...], d_bits)
            qs2[u] = q
            curve = curve + q * v
        return curve, tail

    def seconds(carry, lo, hi):
        steps = (hi - lo) // WIDTH
        carry = lax.fori_loop(0, steps, lambda i, c: second(c, *(lo + WIDTH * i + j for j in range(WIDTH))), carry)
        rest = range(lo + WIDTH * steps, hi)
        return second(carry, *rest) if rest else carry

    carry = (jnp.zeros((1, local), F32), jnp.zeros((1, local - TOP), F32))
    carry = seconds(carry, 2, FAR)
    for u in range(2, FAR):
        to_owner(qs2, qr2, 14, u).start()
    whole(rr, FAR, 16).wait()
    curve, tail = seconds(carry, FAR, UNITS)
    for u in FAR_UNITS:
        if u >= FAR:
            to_owner(qs2, qr2, 14, u).start()
    applied = row_of() + jnp.concatenate([jnp.zeros((1, TOP), F32), tail], axis=1) + weight * d_own
    cc[0] = jnp.where(lane == 0, jnp.sum(d_own * applied + curve), 0.0)
    to_all(cc, 4)
    whole(qs2, 2, 14).wait_send()
    whole(qr2, 2, 14).wait_recv()
    applied = applied + jnp.sum(qr2[2:], axis=0)
    whole(cc, 1, 4).wait()
    step1 = norm1 / jnp.sum(jnp.sum(cc[...], axis=0))
    coef_out[...] = (step0 * target + step1 * d_own).reshape(local)
    res_out[...] = (r1 - step1 * applied).reshape(local)


def body(points, targets, ridge_weight):
    local, dim = points.shape
    dma = pltpu.SemaphoreType.DMA
    vec = jax.ShapeDtypeStruct((local,), F32)
    rows = pltpu.VMEM((UNITS, 1, local), F32)
    small = pltpu.VMEM((128, 1, 128), F32)
    chunks = len(CHUNKS)
    coef, res = pl.pallas_call(
        kernel,
        out_shape=(vec, vec),
        in_specs=[
            pl.BlockSpec(memory_space=pl.ANY),
            pl.BlockSpec(memory_space=pl.ANY),
            pl.BlockSpec(memory_space=pltpu.SMEM),
        ],
        out_specs=(pl.BlockSpec(memory_space=pltpu.VMEM), pl.BlockSpec(memory_space=pltpu.VMEM)),
        scratch_shapes=[
            pltpu.VMEM((1, local), F32),
            pltpu.VMEM((2, SLOTS, dim, local), BF16),
            pltpu.VMEM((2, SLOTS, 1, 2 * local), F32),
            rows, rows, rows, rows, rows, rows, small, small, small,
            pltpu.VMEM((local, 4 * dim), BF16),
            pltpu.VMEM((2, local, 128), F32),
            pltpu.VMEM((UNITS, local, local), BF16),
            pltpu.VMEM((local, local), BF16),
            pltpu.VMEM((local, local), BF16),
            dma, dma((chunks,)), dma((chunks,)), dma((chunks + 1,)), dma((chunks + 1,)), dma((18,)),
            pltpu.SemaphoreType.REGULAR,
        ],
        compiler_params=pltpu.CompilerParams(
            collective_id=0, has_side_effects=True, vmem_limit_bytes=62 * 1024 * 1024),
    )(points.T, targets.reshape(1, local), ridge_weight.reshape(1, 1))
    return coef, res


def solution(mesh):
    return jax.shard_map(
        body, mesh=mesh,
        in_specs=(P("pts", None), P("pts"), P()),
        out_specs=(P("pts"), P("pts")), check_vma=False)
```

```python
import jax
import jax.numpy as jnp
from jax import lax
from jax.experimental import pallas as pl
from jax.experimental.pallas import tpu as pltpu
from jax.sharding import PartitionSpec as P

F32 = jnp.float32
BF16 = jnp.bfloat16
TREE = (
    ((0, 0, 1), 0, 2, 1), ((0, 1, 0), 0, 1, 1), ((1, 0, 0), 0, 0, 1), ((1, 3, 0), 3, 1, -1), ((1, 1, 0), 2, 0, 1),
    ((3, 0, 1), 1, 0, -1), ((0, 1, 1), 1, 1, 1), ((0, 1, 3), 2, 2, -1), ((1, 0, 1), 3, 2, 1), ((0, 1, 2), 8, 2, -1),
    ((3, 0, 2), 6, 2, 1), ((1, 1, 1), 5, 2, 1), ((1, 2, 0), 4, 1, -1), ((1, 3, 3), 4, 2, -1), ((2, 0, 1), 6, 0, -1),
    ((2, 3, 0), 4, 0, 1), ((0, 2, 1), 7, 1, 1), ((1, 1, 3), 5, 2, -1), ((1, 3, 1), 9, 1, -1), ((1, 2, 1), 12, 1, 1),
    ((1, 2, 3), 13, 2, -1), ((3, 1, 2), 10, 0, -1), ((2, 3, 1), 15, 1, -1), ((2, 3, 3), 14, 0, 1), ((3, 3, 2), 11, 1, -1),
    ((2, 2, 1), 20, 0, 1), ((1, 2, 2), 21, 2, -1), ((2, 1, 2), 22, 0, -1), ((0, 0, 2), 1, 2, 1), ((0, 2, 0), 2, 1, 1),
    ((2, 0, 0), 3, 0, 1), ((0, 2, 2), 10, 1, 1), ((2, 0, 2), 11, 0, -1), ((2, 2, 0), 16, 1, -1), ((2, 2, 2), 26, 2, 1))
PLACES = ((0, 0, 0),) + tuple(t[0] for t in TREE)
SLOTS = len(PLACES)
SELF = 29
UNITS = 2 * SELF + SLOTS - SELF
CHUNKS = ((1, 3), (4, 6), (10, 10), (20, 6), (26, 3), (29, 3), (32, 3), (35, 1))
LOG2E = 1.4426950408889634


def plane_of(plane, lo, hi):
    return tuple((s, plane) for s in range(lo, hi))


PLAN = (
    ((0,), (len(CHUNKS),), plane_of(0, 1, 4) + plane_of(0, 0, 1) + plane_of(1, 0, 1)),
    ((), (0,), plane_of(1, 1, 4)),
    ((1,), (), plane_of(0, 4, 10)),
    ((5,), (1,), plane_of(1, 4, 10)),
    ((2,), (5,), plane_of(0, 10, 16)),
    ((), (), plane_of(0, 16, 20) + plane_of(None, 29, 31)),
    ((3,), (2,), plane_of(1, 10, 16)),
    ((6,), (), plane_of(1, 16, 20) + plane_of(None, 31, 32)),
    ((4,), (), plane_of(0, 20, 26)),
    ((), (3, 6), plane_of(1, 20, 26)),
    ((7,), (4,), plane_of(0, 26, 29) + plane_of(1, 26, 29)),
    ((), (7,), plane_of(None, 32, 36)))
ALL = tuple((z, y, x) for z in range(4) for y in range(4) for x in range(4))


def chunk_of(s):
    return [lo <= s < lo + n for lo, n in CHUNKS].index(True)


def hops(m):
    return sum(min(v, 4 - v) for v in m)


def slot_of(u):
    return (u // 2, u % 2) if u < 2 * SELF else (u - SELF, None)


TOP = 384
WIDTH = 4
FAR = 40
FAR_UNITS = sorted(range(2, UNITS), key=lambda u: -hops(PLACES[slot_of(u)[0]]))
FAR_CHIPS = sorted(ALL, key=lambda m: -hops(m))


def kernel(pts_hbm, tgt_hbm, ridge, coef_out, res_out, tgt, bl, tl, tu, rr, qs1, qr1, qs2, qr2, ca, cb, cc,
           own_l, pacc, kt, ka, kb, sem_in, gb, gt, db, dt, sems, ack):
    me = lax.axis_index("pts")
    local = tgt_hbm.shape[1]
    dim = bl.shape[2]
    half = local // 2
    core = lax.rem(me, 2)
    chip = me // 2
    pos = (chip // 16, lax.rem(chip // 4, 4), lax.rem(chip, 4))
    axis = [[lax.rem(pos[d] + a, 4) * (32, 8, 2)[d] for a in range(4)] for d in range(3)]
    cores = (core, 1 - core)
    upper = [p // 2 for p in pos]

    def device(m, c, sign=1):
        return sum(axis[d][sign * m[d] % 4] for d in range(3)) + c

    def split(s):
        return upper[PLACES[s].index(2)]

    partner = device((0, 0, 0), cores[1])
    load = pltpu.make_async_copy(pts_hbm, bl.at[0, 0], sem_in)
    load.start()
    fetch = pltpu.make_async_copy(tgt_hbm, tgt, sems.at[0])
    fetch.start()
    barrier = pltpu.get_barrier_semaphore()
    near = [partner] + [device(tuple(int(d == i) for i in range(3)), core, sign) for d in range(3) for sign in (1, -1)]
    for dev in near:
        pl.semaphore_signal(barrier, inc=1, device_id=(dev,), device_id_type=pl.DeviceIdType.MESH)

    fetch.wait()
    target = tgt[...]
    t_bits = target.astype(BF16)

    load.wait()
    own_t = bl[0, 0].astype(F32)
    norm_row = jnp.sum(own_t * own_t, axis=0, keepdims=True) * (-LOG2E / dim)
    tl[0, 0] = jnp.concatenate([target, norm_row], axis=1)

    def send(src, dst, ssem, rsem, dev):
        return pltpu.make_async_remote_copy(
            src_ref=src, dst_ref=dst, send_sem=ssem, recv_sem=rsem,
            device_id=(dev,), device_id_type=pl.DeviceIdType.MESH)

    def hop(s):
        _, src, d, sign = TREE[s - 1]
        g = chunk_of(s)
        dev = device(tuple(int(d == i) for i in range(3)), core, sign)
        return (send(bl.at[0, src], bl.at[0, s], sems.at[0], gb.at[g], dev),
                send(tl.at[0, src], tl.at[0, s], sems.at[1], gt.at[g], dev))

    def across_chip(s):
        g = chunk_of(s) if s else len(CHUNKS)
        return (send(bl.at[0, s], bl.at[1, s], sems.at[2], db.at[g], partner),
                send(tl.at[0, s], tl.at[1, s], sems.at[3], dt.at[g], partner))

    def start(copies):
        for copy in copies:
            copy.start()

    def arrive(plane, g):
        lo, n = CHUNKS[g] if g < len(CHUNKS) else (0, 1)
        for buf, sem in ((bl, (gb, db)[plane]), (tl, (gt, dt)[plane])):
            ref = buf.at[plane, pl.ds(lo, n)]
            send(ref, ref, sems.at[0], sem.at[g], partner).wait_recv()

    def serve(g):
        arrive(0, g)
        lo, n = CHUNKS[g]
        for s in range(lo, lo + n):
            start(across_chip(s))
        for s in range(1, SLOTS):
            if lo <= TREE[s - 1][1] < lo + n:
                start(hop(s))
        for s in range(lo, min(lo + n, SELF)):
            pl.semaphore_signal(ack, inc=1, device_id=(device(PLACES[s], core, -1),), device_id_type=pl.DeviceIdType.MESH)

    def whole(buf, lo, sem):
        rest = buf.at[pl.ds(lo, buf.shape[0] - lo)]
        return send(rest, rest, sems.at[sem], sems.at[sem + 1], partner)

    def to_owner(qs, qr, sem, u):
        s, plane = slot_of(u)
        c = cores[plane] if plane is not None else lax.rem(core + split(s), 2)
        return send(qs.at[u], qr.at[u], sems.at[sem], sems.at[sem + 1], device(PLACES[s], c, -1))

    def to_user(buf, sem, u):
        s, plane = slot_of(u)
        c = cores[plane] if plane is not None else lax.rem(core + 1 + split(s), 2)
        return send(buf.at[0], buf.at[u], sems.at[sem], sems.at[sem + 1], device(PLACES[s], c))

    def to_all(buf, sem):
        for m in FAR_CHIPS:
            for p in (0, 1):
                if hops(m) + p:
                    at = p * 64 + m[0] * 16 + m[1] * 4 + m[2]
                    send(buf.at[0], buf.at[at], sems.at[sem], sems.at[sem + 1], device(m, cores[p])).start()

    pl.semaphore_wait(barrier, len(near))
    for s in range(1, SLOTS):
        if TREE[s - 1][1] == 0:
            start(hop(s))
    start(across_chip(0))

    def three(x):
        hi = x.astype(BF16).astype(F32)
        mid = (x - hi).astype(BF16).astype(F32)
        return hi, mid, x - hi - mid

    def tagged(lead, then):
        rows = lax.broadcasted_iota(jnp.int32, (8, local), 0)
        out = jnp.zeros((8, local), F32)
        for i, x in enumerate(lead + then):
            out = jnp.where(rows == i, x, out)
        return jnp.concatenate([out, jnp.zeros((8, local), F32)], axis=0)

    ones = (1.0, 1.0, 1.0)
    left = jnp.concatenate([*three(own_t * (2.0 * LOG2E / dim)), tagged(ones, three(norm_row)),
                            jnp.zeros((dim - 16, local), F32)], axis=0)
    own_l[...] = left.T.astype(BF16)
    rest = jnp.zeros((dim - 16, local), BF16)

    def power(u, plane, s):
        row = tl[plane, s]
        tu[u] = row[:, :local]
        pb = bl[plane, s]
        tags = tagged(three(row[:, local:]), ones).astype(BF16)
        right = jnp.concatenate([pb, pb, pb, tags, rest], axis=0)
        return jnp.dot(own_l[...], right, preferred_element_type=F32)

    def keep(u, e, side):
        for r in range(0, local, 32):
            k = jnp.exp2(e[r:r + 32]).astype(BF16)
            kt[u, r:r + 32] = k
            (ka, kb)[side][r:r + 32] = k

    def down(k, bits):
        return jnp.dot(bits, k, preferred_element_type=F32)

    def across(acc, *pairs, rows=None):
        lows = [v.astype(BF16).astype(F32) for _, v in pairs]
        for r in range(0, rows or local, 16):
            cut = pl.ds(r, 16)
            total = acc[cut]
            for (k, _), low in zip(pairs, lows):
                for c in range(0, local, 128):
                    total = total + k[cut, c:c + 128].astype(F32) * low[:, c:c + 128]
            acc[cut] = total

    def row_of():
        return jnp.sum((pacc[0] + pacc[1]).T, axis=0, keepdims=True)

    def absorb(u, side, tw):
        held = (ka, kb)[side]
        v = tu[u]
        q = None
        if u > 1:
            q = down(held[...], t_bits)
            qs1[u] = q
        across(pacc.at[side], (held, v))
        return tw if q is None else tw + q * v

    pacc[...] = jnp.zeros_like(pacc)
    tw = jnp.zeros((1, local), F32)
    sent, ready = [], []

    def send_ready():
        for u in ready:
            to_owner(qs1, qr1, 8, u).start()
        sent.extend(ready)
        ready.clear()

    prev, count = None, 1
    for served, crossed, units in PLAN:
        for g in served:
            serve(g)
        for g in crossed:
            arrive(1, g)
        send_ready()
        units = [(s + SELF, split(s), s) if plane is None else (2 * s + plane, plane, s) for s, plane in units]
        e = power(*units[0])
        for j, (u, _, _) in enumerate(units):
            ahead = power(*units[j + 1]) if j + 1 < len(units) else None
            if prev is not None:
                tw = absorb(prev, count % 2, tw)
                if prev > 1:
                    ready.append(prev)
            count += 1
            keep(u, e, count % 2)
            prev, e = u, ahead

    tw = absorb(prev, count % 2, tw)
    ready.append(prev)

    ready.reverse()
    send_ready()
    weight = ridge[0, 0]
    base = row_of() + weight * target
    lane = lax.broadcasted_iota(jnp.int32, (1, 128), 1)
    ca[0] = jnp.where(lane == 0, jnp.sum(tw + target * base), jnp.where(lane == 1, jnp.sum(target * target), 0.0))
    pl.semaphore_wait(ack, SELF - 1)
    to_all(ca, 6)
    moved = bl.at[0, pl.ds(1, SLOTS - 1)], tl.at[0, pl.ds(1, SLOTS - 1)], bl.at[0], tl.at[0]
    for i, ref in enumerate(moved):
        send(ref, ref, sems.at[i], sem_in, partner).wait_send()
    whole(qs1, 2, 8).wait_send()
    whole(qr1, 2, 8).wait_recv()
    w = base + jnp.sum(qr1[2:], axis=0)
    whole(ca, 1, 6).wait()
    sums = jnp.sum(ca[...], axis=0)
    norm0 = jnp.sum(sums[:, 1:2])
    step0 = norm0 / jnp.sum(sums[:, 0:1])
    r1 = target - step0 * w
    rr[0] = r1
    cb[0] = jnp.where(lane == 0, jnp.sum(r1 * r1), 0.0)
    to_all(cb, 12)
    for u in FAR_UNITS:
        to_user(rr, 16 if u >= FAR else 10, u).start()
    send(rr.at[0], rr.at[1], sems.at[10], sems.at[11], partner).start()
    whole(cb, 1, 12).wait()
    norm1 = jnp.sum(jnp.sum(cb[...], axis=0))
    beta = norm1 / norm0
    whole(rr.at[pl.ds(0, FAR)], 1, 10).wait()

    d_own = r1 + beta * target
    d_bits = d_own.astype(BF16)
    pacc[...] = jnp.zeros_like(pacc)

    def again(u):
        return kt.at[u], rr[u] + beta * tu[u]

    across(pacc.at[0], again(0), again(1))

    def second(carry, *units):
        curve, tail = carry
        pairs = [again(u) for u in units]
        for k, v in pairs:
            tail = tail + lax.dot_general(v.astype(BF16), k[TOP:], (((1,), (1,)), ((), ())), preferred_element_type=F32)
        across(pacc.at[0], *pairs, rows=TOP)
        for u, (k, v) in zip(units, pairs):
            q = down(k[...], d_bits)
            qs2[u] = q
            curve = curve + q * v
        return curve, tail

    def seconds(carry, lo, hi):
        steps = (hi - lo) // WIDTH
        carry = lax.fori_loop(0, steps, lambda i, c: second(c, *(lo + WIDTH * i + j for j in range(WIDTH))), carry)
        rest = range(lo + WIDTH * steps, hi)
        return second(carry, *rest) if rest else carry

    carry = (jnp.zeros((1, local), F32), jnp.zeros((1, local - TOP), F32))
    carry = seconds(carry, 2, FAR)
    for u in range(2, FAR):
        to_owner(qs2, qr2, 14, u).start()
    whole(rr, FAR, 16).wait()
    curve, tail = seconds(carry, FAR, UNITS)
    for u in FAR_UNITS:
        if u >= FAR:
            to_owner(qs2, qr2, 14, u).start()
    applied = row_of() + jnp.concatenate([jnp.zeros((1, TOP), F32), tail], axis=1) + weight * d_own
    cc[0] = jnp.where(lane == 0, jnp.sum(d_own * applied + curve), 0.0)
    to_all(cc, 4)
    whole(qs2, 2, 14).wait_send()
    whole(qr2, 2, 14).wait_recv()
    applied = applied + jnp.sum(qr2[2:], axis=0)
    whole(cc, 1, 4).wait()
    step1 = norm1 / jnp.sum(jnp.sum(cc[...], axis=0))
    coef_out[...] = (step0 * target + step1 * d_own).reshape(local)
    res_out[...] = (r1 - step1 * applied).reshape(local)


def body(points, targets, ridge_weight):
    local, dim = points.shape
    dma = pltpu.SemaphoreType.DMA
    vec = jax.ShapeDtypeStruct((local,), F32)
    rows = pltpu.VMEM((UNITS, 1, local), F32)
    small = pltpu.VMEM((128, 1, 128), F32)
    chunks = len(CHUNKS)
    coef, res = pl.pallas_call(
        kernel,
        out_shape=(vec, vec),
        in_specs=[
            pl.BlockSpec(memory_space=pl.ANY),
            pl.BlockSpec(memory_space=pl.ANY),
            pl.BlockSpec(memory_space=pltpu.SMEM),
        ],
        out_specs=(pl.BlockSpec(memory_space=pltpu.VMEM), pl.BlockSpec(memory_space=pltpu.VMEM)),
        scratch_shapes=[
            pltpu.VMEM((1, local), F32),
            pltpu.VMEM((2, SLOTS, dim, local), BF16),
            pltpu.VMEM((2, SLOTS, 1, 2 * local), F32),
            rows, rows, rows, rows, rows, rows, small, small, small,
            pltpu.VMEM((local, 4 * dim), BF16),
            pltpu.VMEM((2, local, 128), F32),
            pltpu.VMEM((UNITS, local, local), BF16),
            pltpu.VMEM((local, local), BF16),
            pltpu.VMEM((local, local), BF16),
            dma, dma((chunks,)), dma((chunks,)), dma((chunks + 1,)), dma((chunks + 1,)), dma((18,)),
            pltpu.SemaphoreType.REGULAR,
        ],
        compiler_params=pltpu.CompilerParams(
            collective_id=0, has_side_effects=True, vmem_limit_bytes=62 * 1024 * 1024),
    )(points.T, targets.reshape(1, local), ridge_weight.reshape(1, 1))
    return coef, res


def solution(mesh):
    return jax.shard_map(
        body, mesh=mesh,
        in_specs=(P("pts", None), P("pts"), P()),
        out_specs=(P("pts"), P("pts")), check_vma=False)
```
